16 devices in a mesh: dp: 2 (over y, z), tp: 8 (over x, core).
Axes of the slice: x: 4, y: 2, z: 1, core: 2. Of those that a mesh axis runs over, the one named last changes fastest.
The devices are a block of a 4x4x8 slice.
Arguments:
- x_in: bfloat16 [3072, 2048], P('dp'), parts along dimension 0
- g_norm: bfloat16 [2048], replicated
- w_q: bfloat16 [2048, 2048], P(None, 'tp')
- w_k: bfloat16 [2048, 1024], replicated
- w_v: bfloat16 [2048, 1024], replicated
- w_o: bfloat16 [2048, 2048], P('tp')
- w_gate: bfloat16 [2048, 6144], P(None, 'tp')
- w_up: bfloat16 [2048, 6144], P(None, 'tp')
- w_down: bfloat16 [6144, 2048], P('tp')
Outputs:
- output 1: bfloat16 [3072, 2048], P('dp'), parts along dimension 0
- output 2: bfloat16 [3072, 8, 128], P('dp', 'tp'), parts along dimension 0
- output 3: bfloat16 [3072, 8, 128], P('dp', 'tp'), parts along dimension 0
There are 2 independent parts. The reference program is written for one: setup_inputs(seed, part) draws one part's arguments, and reference() takes and returns one part's arrays. A program takes and returns all parts, laid end to end along the dimension named above; an argument that names none is the same for every part.
All inputs are finite; a program needn't handle non-finite values.
Results may differ from the reference program's by a relative error of at most 0.0121325.
Values are sent between devices in bfloat16 or wider.
A program may use at most 768 MiB of HBM per device.

```python
import math
import jax
import jax.numpy as jnp
from jax import lax

TOKENS = 1536
D = 2048
HEADS = 16
KV_HEADS = 8
HEAD = 128
FF = 6144
KV_SLOTS = 8
QBLOCK = 128

ROPE_BASE = 500000.0
NORM_EPS = 1e-5


def setup_inputs(seed: int = 0, part: int = 0) -> dict:
    key_list = jax.random.split(jax.random.key(seed), 10)
    part_key = jax.random.fold_in(key_list[9], part)
    q_gain = math.sqrt(math.log(TOKENS / 16.0)) / 1.09
    x_val = 0.7 * jax.random.normal(part_key, (TOKENS, D), jnp.float32)
    g_val = jnp.exp(0.7 * jax.random.normal(key_list[0], (D,), jnp.float32) - 0.49)
    w_q = jax.random.normal(key_list[1], (D, HEADS * HEAD), jnp.float32) * (q_gain / math.sqrt(D))
    w_k = jax.random.normal(key_list[2], (D, KV_HEADS * HEAD), jnp.float32) / math.sqrt(D)
    w_v = jax.random.normal(key_list[3], (D, KV_HEADS * HEAD), jnp.float32) / math.sqrt(D)
    w_o = jax.random.normal(key_list[4], (HEADS * HEAD, D), jnp.float32) * (3.0 / math.sqrt(HEADS * HEAD))
    w_gate = jax.random.normal(key_list[5], (D, FF), jnp.float32) / math.sqrt(D)
    w_up = jax.random.normal(key_list[6], (D, FF), jnp.float32) / math.sqrt(D)
    w_down = jax.random.normal(key_list[7], (FF, D), jnp.float32) / math.sqrt(FF)
    return {'x_in': x_val.astype(jnp.bfloat16), 'g_norm': g_val.astype(jnp.bfloat16), 'w_q': w_q.astype(jnp.bfloat16), 'w_k': w_k.astype(jnp.bfloat16), 'w_v': w_v.astype(jnp.bfloat16), 'w_o': w_o.astype(jnp.bfloat16), 'w_gate': w_gate.astype(jnp.bfloat16), 'w_up': w_up.astype(jnp.bfloat16), 'w_down': w_down.astype(jnp.bfloat16)}


def rope_tables(positions):
    inv_freq = ROPE_BASE ** (-jnp.arange(0, HEAD, 2, dtype=jnp.float32) / HEAD)
    angles = positions.astype(jnp.float32)[:, None] * inv_freq[None, :]
    return jnp.cos(angles), jnp.sin(angles)


def apply_rope(projected, cos_tab, sin_tab):
    half_dim = HEAD // 2
    lower_half = projected[..., :half_dim]
    upper_half = projected[..., half_dim:]
    cos_b = cos_tab[:, None, :]
    sin_b = sin_tab[:, None, :]
    return jnp.concatenate([lower_half * cos_b - upper_half * sin_b, upper_half * cos_b + lower_half * sin_b], axis=-1)


def reference(x_in, g_norm, w_q, w_k, w_v, w_o, w_gate, w_up, w_down):
    x_f32 = x_in.astype(jnp.float32)
    inv_rms = lax.rsqrt(jnp.mean(x_f32 * x_f32, axis=-1, keepdims=True) + NORM_EPS)
    normed = (x_f32 * inv_rms * g_norm.astype(jnp.float32)).astype(jnp.bfloat16)
    cos_tab, sin_tab = rope_tables(jnp.arange(TOKENS))
    q_proj = jnp.dot(normed, w_q, preferred_element_type=jnp.float32).reshape(TOKENS, HEADS, HEAD)
    k_proj = jnp.dot(normed, w_k, preferred_element_type=jnp.float32).reshape(TOKENS, KV_HEADS, HEAD)
    q_rot = apply_rope(q_proj, cos_tab, sin_tab).astype(jnp.bfloat16)
    k_rot = apply_rope(k_proj, cos_tab, sin_tab).astype(jnp.bfloat16)
    v_proj = jnp.dot(normed, w_v, preferred_element_type=jnp.float32).astype(jnp.bfloat16).reshape(TOKENS, KV_HEADS, HEAD)
    group_size = HEADS // KV_HEADS
    q_grouped = q_rot.reshape(TOKENS, KV_HEADS, group_size, HEAD)
    k_f32 = k_rot.astype(jnp.float32)
    v_f32 = v_proj.astype(jnp.float32)
    score_scale = 1.0 / math.sqrt(HEAD)
    key_pos = jnp.arange(TOKENS)

    def attend_block(block_idx):
        row_start = block_idx * QBLOCK
        q_part = lax.dynamic_slice_in_dim(q_grouped, row_start, QBLOCK, axis=0).astype(jnp.float32)
        scores = jnp.einsum('qgrd,kgd->grqk', q_part, k_f32) * score_scale
        query_pos = row_start + jnp.arange(QBLOCK)
        visible = key_pos[None, :] <= query_pos[:, None]
        scores = jnp.where(visible, scores, -1e30)
        probs = jax.nn.softmax(scores, axis=-1).astype(jnp.bfloat16).astype(jnp.float32)
        return jnp.einsum('grqk,kgd->qgrd', probs, v_f32).astype(jnp.bfloat16)

    attn_blocks = lax.map(attend_block, jnp.arange(TOKENS // QBLOCK))
    attn_out = attn_blocks.reshape(TOKENS, HEADS * HEAD)
    attn_sum = jnp.dot(attn_out, w_o, preferred_element_type=jnp.float32)
    gate_proj = jnp.dot(normed, w_gate, preferred_element_type=jnp.float32)
    up_proj = jnp.dot(normed, w_up, preferred_element_type=jnp.float32)
    hidden = (jax.nn.silu(gate_proj) * up_proj).astype(jnp.bfloat16)
    mlp_sum = jnp.dot(hidden, w_down, preferred_element_type=jnp.float32)
    y_out = (x_f32 + attn_sum + mlp_sum).astype(jnp.bfloat16)
    slot_repeat = KV_SLOTS // KV_HEADS
    k_cache = jnp.repeat(k_rot, slot_repeat, axis=1)
    v_cache = jnp.repeat(v_proj, slot_repeat, axis=1)
    return (y_out, k_cache, v_cache)
```

```python
import functools
import math
import numpy as np
import jax
import jax.numpy as jnp
from jax import lax
from jax.experimental import pallas as pl
from jax.experimental.pallas import tpu as pltpu
from jax.sharding import PartitionSpec as P

HEAD_DIM = 128
ROPE_BASE = 500000.0
NORM_EPS = 1e-5
ROWS = 256
KEYS = 256
TILE = 256
F32 = jnp.float32
BF16 = jnp.bfloat16
MESH = pl.DeviceIdType.MESH

(SWAP, FWD_R, OWN_R, FWD_L, OWN_L, SUM_R, SUM_L, OUT_R, OUT_L, OUT_P, FAR_R, FAR_L,
 P_LEFT, P_RIGHT, P_FAR_A, P_FAR_B) = range(16)
N_KINDS = 16


def rope_constants(rows, blocks):
    inv_freq = ROPE_BASE ** (-np.arange(0, HEAD_DIM, 2, dtype=np.float64) / HEAD_DIM)
    def tables(positions):
        ang = positions[:, None] * inv_freq[None, :]
        cos, sin = np.cos(ang), np.sin(ang)
        return (np.concatenate([cos, cos], 1).astype(np.float32),
                np.concatenate([-sin, sin], 1).astype(np.float32))
    cos_r, sin_r = tables(np.arange(rows, dtype=np.float64))
    cos_t, sin_t = tables(np.arange(blocks, dtype=np.float64) * rows)
    return cos_r, sin_r, cos_t, sin_t


def layer_kernel(n_tp, x_hbm, g_ref, wq_hbm, wk_hbm, wv_hbm, wo_hbm, wg_hbm, wu_hbm, wd_hbm,
                 cos_r, sin_r, cos_t, sin_t, y_ref, k_ref, v_ref,
                 x_v, wqkv, wgu, wod, a_s, q_s, s_s, m_s, l_s, o_s, om_s, part, swap, fwd, from_l, from_r,
                 load_sem, send_sem, recv_sem):
    tokens, width = x_v.shape
    blocks = tokens // ROWS
    half = ROWS // 2
    n_chip = n_tp // 2
    chunk = half // n_chip
    wh = width // 2
    qw = wq_hbm.shape[1]
    heads = qw // HEAD_DIM
    ff = wg_hbm.shape[1]
    me = lax.axis_index('tp')
    chip, core = me // 2, lax.rem(me, 2)
    partner = chip * 2 + 1 - core
    c_r = lax.rem(chip + 1, n_chip)
    c_l = lax.rem(chip + n_chip - 1, n_chip)
    c_o = lax.rem(chip + 2, n_chip)
    right = c_r * 2 + core
    left = c_l * 2 + core

    kv_col = pl.multiple_of(me * HEAD_DIM, HEAD_DIM)
    def x_load(t):
        rows = pl.ds(pl.multiple_of(t * ROWS, ROWS), ROWS)
        return pltpu.make_async_copy(x_hbm.at[rows], x_v.at[rows], load_sem.at[8 + t])
    w_loads = [
        pltpu.make_async_copy(wq_hbm, wqkv.at[:, pl.ds(0, qw)], load_sem.at[0]),
        pltpu.make_async_copy(wk_hbm.at[:, pl.ds(kv_col, HEAD_DIM)], wqkv.at[:, pl.ds(qw, HEAD_DIM)], load_sem.at[1]),
        pltpu.make_async_copy(wv_hbm.at[:, pl.ds(kv_col, HEAD_DIM)], wqkv.at[:, pl.ds(qw + HEAD_DIM, HEAD_DIM)], load_sem.at[2]),
        pltpu.make_async_copy(wg_hbm, wgu.at[:, pl.ds(0, ff)], load_sem.at[3]),
        pltpu.make_async_copy(wu_hbm, wgu.at[:, pl.ds(ff, ff)], load_sem.at[4]),
        pltpu.make_async_copy(wo_hbm, wod.at[pl.ds(0, qw)], load_sem.at[5]),
        pltpu.make_async_copy(wd_hbm, wod.at[pl.ds(qw, ff)], load_sem.at[6]),
    ]
    x_load(0).start()
    for cp in w_loads:
        cp.start()
    for t in range(1, blocks):
        x_load(t).start()

    barrier = pltpu.get_barrier_semaphore()
    for dev in (partner, left, right):
        pl.semaphore_signal(barrier, inc=1, device_id={'tp': dev}, device_id_type=MESH)
    k_ref[...] = jnp.zeros_like(k_ref)
    v_ref[...] = jnp.zeros_like(v_ref)
    pl.semaphore_wait(barrier, 3)

    def rows_of(t, c):
        return pl.ds(pl.multiple_of(t * ROWS + core * half + c * chunk, chunk), chunk)

    def slot(t):
        return pl.ds(pl.multiple_of(t * chunk, chunk), chunk)

    A, B = pl.ds(0, wh), pl.ds(wh, wh)

    def copy(kind, t):
        other = pl.ds(pl.multiple_of(t * ROWS + (1 - core) * half, half), half)
        src, dst, dev = {
            SWAP: lambda: (part.at[other], swap.at[pl.ds(pl.multiple_of(t * half, half), half)], partner),
            FWD_R: lambda: (part.at[rows_of(t, c_o), A], fwd.at[slot(t), A], right),
            OWN_R: lambda: (part.at[rows_of(t, c_r), B], from_l.at[slot(t), B], right),
            FWD_L: lambda: (part.at[rows_of(t, c_o), B], fwd.at[slot(t), B], left),
            OWN_L: lambda: (part.at[rows_of(t, c_l), A], from_r.at[slot(t), A], left),
            SUM_R: lambda: (part.at[rows_of(t, c_r), A], from_l.at[slot(t), A], right),
            SUM_L: lambda: (part.at[rows_of(t, c_l), B], from_r.at[slot(t), B], left),
            OUT_R: lambda: (y_ref.at[rows_of(t, chip)], y_ref.at[rows_of(t, chip)], right),
            OUT_L: lambda: (y_ref.at[rows_of(t, chip)], y_ref.at[rows_of(t, chip)], left),
            OUT_P: lambda: (y_ref.at[rows_of(t, chip)], y_ref.at[rows_of(t, chip)], partner),
            FAR_R: lambda: (y_ref.at[rows_of(t, c_l), A], y_ref.at[rows_of(t, c_l), A], right),
            FAR_L: lambda: (y_ref.at[rows_of(t, c_r), B], y_ref.at[rows_of(t, c_r), B], left),
            P_LEFT: lambda: (y_ref.at[rows_of(t, c_l)], y_ref.at[rows_of(t, c_l)], partner),
            P_RIGHT: lambda: (y_ref.at[rows_of(t, c_r)], y_ref.at[rows_of(t, c_r)], partner),
            P_FAR_A: lambda: (y_ref.at[rows_of(t, c_o), A], y_ref.at[rows_of(t, c_o), A], partner),
            P_FAR_B: lambda: (y_ref.at[rows_of(t, c_o), B], y_ref.at[rows_of(t, c_o), B], partner),
        }[kind]()
        return pltpu.make_async_remote_copy(
            src_ref=src, dst_ref=dst, send_sem=send_sem.at[kind, t], recv_sem=recv_sem.at[kind, t],
            device_id={'tp': dev}, device_id_type=MESH)

    scale = 1.0 / math.sqrt(HEAD_DIM) * math.log2(math.e)

    def project(t):
        x_load(t).wait()
        step = 64
        for i in range(ROWS // step):
            xf = x_v[pl.ds(pl.multiple_of(t * ROWS + i * step, step), step), :].astype(F32)
            inv = lax.rsqrt(jnp.mean(xf * xf, axis=-1, keepdims=True) + NORM_EPS)
            a_s[pl.ds(i * step, step), :] = (xf * inv * g_ref[...].astype(F32)).astype(BF16)

        @pl.when(t == 0)
        def _():
            for cp in w_loads[:3]:
                cp.wait()
        a = a_s[...]
        c0, s0 = cos_t[pl.ds(t, 1), :], sin_t[pl.ds(t, 1), :]
        cos = cos_r[...] * c0 - sin_r[...] * s0
        sin = sin_r[...] * c0 + cos_r[...] * s0
        rot = lambda p: (p * cos + pltpu.roll(p, HEAD_DIM // 2, 1) * sin).astype(BF16)
        q = jnp.dot(a, wqkv[:, pl.ds(0, qw)], preferred_element_type=F32)
        kv = jnp.dot(a, wqkv[:, pl.ds(qw, 2 * HEAD_DIM)], preferred_element_type=F32)
        for h in range(heads):
            q_s[pl.ds(h * ROWS, ROWS), :] = rot(q[:, h * HEAD_DIM:(h + 1) * HEAD_DIM])
        rows = pl.ds(pl.multiple_of(t * ROWS, ROWS), ROWS)
        k_ref[rows, :] = rot(kv[:, :HEAD_DIM])
        v_ref[rows, :] = kv[:, HEAD_DIM:].astype(BF16)

    def lanes(op, s):
        acc = s[:, :128]
        for i in range(1, KEYS // 128):
            acc = op(acc, s[:, i * 128:(i + 1) * 128])
        return acc

    def attend(t):
        last = (t * ROWS) // KEYS

        def keys(kb):
            return pl.ds(pl.multiple_of(kb * KEYS, KEYS), KEYS)

        def score(kb):
            return lax.dot_general(q_s[...], k_ref[keys(kb), :], (((1,), (1,)), ((), ())), preferred_element_type=F32)

        s = score(last)
        shape = (heads, ROWS, KEYS)
        q_pos = t * ROWS + lax.broadcasted_iota(jnp.int32, shape, 1).reshape(heads * ROWS, KEYS)
        k_pos = last * KEYS + lax.broadcasted_iota(jnp.int32, shape, 2).reshape(heads * ROWS, KEYS)
        s = jnp.where(k_pos <= q_pos, s, -1e30)
        s_s[last] = s
        m_s[...] = lanes(jnp.maximum, s)

        def pass1(kb, _):
            s = score(kb)
            s_s[kb] = s
            m_s[...] = jnp.maximum(m_s[...], lanes(jnp.maximum, s))
            return 0
        lax.fori_loop(0, last, pass1, 0)
        m_s[...] = jnp.broadcast_to(jnp.max(m_s[...], axis=-1, keepdims=True) * scale, m_s.shape)
        l_s[...] = jnp.zeros_like(l_s)

        def pass2(kb, _):
            m = m_s[...]
            p = jnp.exp2(s_s[kb] * scale - jnp.concatenate([m] * (KEYS // 128), axis=1))
            s_s[kb] = p
            l_s[...] += lanes(jnp.add, p)
            return 0
        lax.fori_loop(0, last + 1, pass2, 0)
        l_s[...] = jnp.broadcast_to(1.0 / jnp.sum(l_s[...], axis=-1, keepdims=True), l_s.shape)
        o_s[...] = jnp.zeros_like(o_s)

        def pass3(kb, _):
            r = l_s[...]
            p = (s_s[kb] * jnp.concatenate([r] * (KEYS // 128), axis=1)).astype(BF16)
            o_s[...] += jnp.dot(p, v_ref[keys(kb), :], preferred_element_type=F32)
            return 0
        lax.fori_loop(0, last + 1, pass3, 0)
        for h in range(heads):
            om_s[:, pl.ds(h * HEAD_DIM, HEAD_DIM)] = o_s[pl.ds(h * ROWS, ROWS), :].astype(BF16)

    def mlp(t):
        @pl.when(t == 0)
        def _():
            for cp in w_loads[3:5]:
                cp.wait()
        a = a_s[...]
        for j in range(ff // TILE):
            gate = jnp.dot(a, wgu[:, pl.ds(j * TILE, TILE)], preferred_element_type=F32)
            up = jnp.dot(a, wgu[:, pl.ds(ff + j * TILE, TILE)], preferred_element_type=F32)
            om_s[:, pl.ds(qw + j * TILE, TILE)] = (jax.nn.silu(gate) * up).astype(BF16)

    def out_half(t, which):
        row0 = pl.multiple_of(which * half, half)
        om = om_s[pl.ds(row0, half), :]
        rows = pl.ds(pl.multiple_of(t * ROWS + which * half, half), half)
        for j in range(width // TILE):
            cols = pl.ds(j * TILE, TILE)
            part[rows, cols] = jnp.dot(om, wod[:, cols], preferred_element_type=F32).astype(BF16)

    def chip_sum(t):
        copy(SWAP, t).wait_recv()
        for i in range(4):
            n = half // 4
            rows = pl.ds(pl.multiple_of(t * ROWS + core * half + i * n, n), n)
            got = swap[pl.ds(pl.multiple_of(t * half + i * n, n), n), :].astype(F32)
            part[rows, :] = (part[rows, :].astype(F32) + got).astype(BF16)
        for kind in (FWD_R, FWD_L, OWN_R, OWN_L):
            copy(kind, t).start()

    def pass_on(t):
        for kind, out, c, cols in ((FWD_R, SUM_R, c_r, A), (FWD_L, SUM_L, c_l, B)):
            copy(kind, t).wait_recv()
            rows = rows_of(t, c)
            part[rows, cols] = (part[rows, cols].astype(F32) + fwd[slot(t), cols].astype(F32)).astype(BF16)
            copy(out, t).start()

    def finish(t):
        for kind in (OWN_R, OWN_L, SUM_R, SUM_L):
            copy(kind, t).wait_recv()
        rows = rows_of(t, chip)
        total = (part[rows, :].astype(F32) + from_l[slot(t), :].astype(F32)) + from_r[slot(t), :].astype(F32)
        y_ref[rows, :] = (x_v[rows, :].astype(F32) + total).astype(BF16)
        for kind in (OUT_R, OUT_L, OUT_P):
            copy(kind, t).start()

    def spread(t):
        copy(OUT_R, t).wait_recv()
        copy(FAR_R, t).start()
        copy(P_LEFT, t).start()
        copy(OUT_L, t).wait_recv()
        copy(FAR_L, t).start()
        copy(P_RIGHT, t).start()

    def far(t):
        copy(FAR_R, t).wait_recv()
        copy(P_FAR_A, t).start()
        copy(FAR_L, t).wait_recv()
        copy(P_FAR_B, t).start()

    def close(t):
        for kind in (OUT_P, P_LEFT, P_RIGHT, P_FAR_A, P_FAR_B):
            copy(kind, t).wait_recv()
        for kind in range(N_KINDS):
            copy(kind, t).wait_send()

    def at(t, fn):
        @pl.when(jnp.logical_and(t >= 0, t < blocks))
        def _():
            fn(t)

    def step(s, _):
        @pl.when(s < blocks)
        def _():
            project(s)
            attend(s)
            mlp(s)

            @pl.when(s == 0)
            def _():
                for cp in w_loads[5:]:
                    cp.wait()
            out_half(s, 1 - core)
            copy(SWAP, s).start()
            out_half(s, core)
            chip_sum(s)
        at(s - 1, pass_on)
        at(s - 2, finish)
        at(s - 3, spread)
        at(s - 4, far)
        at(s - 5, close)
        return 0

    lax.fori_loop(0, blocks + 5, step, 0)


def solution(mesh):
    n_tp = mesh.shape['tp']

    def local_layer(x_in, g_norm, w_q, w_k, w_v, w_o, w_gate, w_up, w_down):
        tokens, width = x_in.shape
        blocks = tokens // ROWS
        qw, ff = w_q.shape[1], w_gate.shape[1]
        heads = qw // HEAD_DIM
        half = ROWS // 2
        chunk = half // (n_tp // 2)
        consts = [jnp.asarray(c) for c in rope_constants(ROWS, blocks)]
        vm = lambda: pl.BlockSpec(memory_space=pltpu.VMEM)
        hbm = lambda: pl.BlockSpec(memory_space=pl.ANY)
        y_out, k_rot, v_proj = pl.pallas_call(
            functools.partial(layer_kernel, n_tp),
            out_shape=(jax.ShapeDtypeStruct((tokens, width), BF16),
                       jax.ShapeDtypeStruct((tokens, HEAD_DIM), BF16),
                       jax.ShapeDtypeStruct((tokens, HEAD_DIM), BF16)),
            in_specs=[hbm(), vm()] + [hbm()] * 7 + [vm()] * 4,
            out_specs=(vm(), vm(), vm()),
            scratch_shapes=[
                pltpu.VMEM((tokens, width), BF16),
                pltpu.VMEM((width, qw + 2 * HEAD_DIM), BF16),
                pltpu.VMEM((width, 2 * ff), BF16),
                pltpu.VMEM((qw + ff, width), BF16),
                pltpu.VMEM((ROWS, width), BF16),
                pltpu.VMEM((heads * ROWS, HEAD_DIM), BF16),
                pltpu.VMEM((tokens // KEYS, heads * ROWS, KEYS), F32),
                pltpu.VMEM((heads * ROWS, 128), F32),
                pltpu.VMEM((heads * ROWS, 128), F32),
                pltpu.VMEM((heads * ROWS, HEAD_DIM), F32),
                pltpu.VMEM((ROWS, qw + ff), BF16),
                pltpu.VMEM((tokens, width), BF16),
                pltpu.VMEM((tokens // 2, width), BF16),
                pltpu.VMEM((blocks * chunk, width), BF16),
                pltpu.VMEM((blocks * chunk, width), BF16),
                pltpu.VMEM((blocks * chunk, width), BF16),
                pltpu.SemaphoreType.DMA((8 + blocks,)),
                pltpu.SemaphoreType.DMA((N_KINDS, blocks)),
                pltpu.SemaphoreType.DMA((N_KINDS, blocks)),
            ],
            compiler_params=pltpu.CompilerParams(
                collective_id=0, has_side_effects=True, vmem_limit_bytes=67043328),
            name='layer',
        )(x_in, g_norm.reshape(1, width), w_q, w_k, w_v, w_o, w_gate, w_up, w_down, *consts)
        return y_out, k_rot.reshape(tokens, 1, HEAD_DIM), v_proj.reshape(tokens, 1, HEAD_DIM)

    return jax.shard_map(local_layer, mesh=mesh, in_specs=(P('dp', None), P(None), P(None, 'tp'), P(None, None), P(None, None), P('tp', None), P(None, 'tp'), P(None, 'tp'), P('tp', None)), out_specs=(P('dp', None), P('dp', 'tp', None), P('dp', 'tp', None)), check_vma=False)
```

```python
import functools
import math
import numpy as np
import jax
import jax.numpy as jnp
from jax import lax
from jax.experimental import pallas as pl
from jax.experimental.pallas import tpu as pltpu
from jax.sharding import PartitionSpec as P

HEAD_DIM = 128
ROPE_BASE = 500000.0
NORM_EPS = 1e-5
ROWS = 256
TILE = 256
STORES = 8
F32 = jnp.float32
BF16 = jnp.bfloat16
MESH = pl.DeviceIdType.MESH

(SWAP_A, SWAP_B, FWD_R, OWN_L, FWD_L, OWN_R, SUM_R, SUM_L, OUT_R, OUT_L, OUT_P, FAR_R, FAR_L,
 P_LEFT, P_RIGHT, P_FAR_A, P_FAR_B) = range(17)
N_KINDS = 17

PLACES = {'start': (('pass_on_b', 2),),
          'project': (('chip_sum_a', 1), ('spread', 4), ('close', 7),),
          'values': (('chip_sum_b', 1),),
          'mlp1': (('finish', 2),),
          'out1': (('pass_on_a', 1), ('far', 4),)}
DRAIN = (('spread', 3), ('close', 5), ('chip_sum_a', 0), ('chip_sum_b', 0),
         ('pass_on_b', 1), ('close', 4), ('spread', 2), ('far', 3),
         ('pass_on_a', 0), ('close', 3), ('pass_on_b', 0), ('finish', 1),
         ('far', 2), ('close', 2), ('finish', 0), ('spread', 1),
         ('spread', 0), ('far', 1), ('close', 1), ('far', 0),
         ('close', 0),)


def rope_constants(rows, blocks):
    inv_freq = ROPE_BASE ** (-np.arange(0, HEAD_DIM, 2, dtype=np.float64) / HEAD_DIM)
    def tables(positions):
        ang = positions[:, None] * inv_freq[None, :]
        cos, sin = np.cos(ang), np.sin(ang)
        return (np.concatenate([cos, cos], 1).astype(np.float32),
                np.concatenate([-sin, sin], 1).astype(np.float32))
    cos_r, sin_r = tables(np.arange(rows, dtype=np.float64))
    cos_t, sin_t = tables(np.arange(blocks, dtype=np.float64) * rows)
    return cos_r, sin_r, cos_t, sin_t


def layer_kernel(n_tp, x_hbm, g_hbm, wq_hbm, wk_hbm, wv_hbm, wo_hbm, wg_hbm, wu_hbm, wd_hbm,
                 rope_r_hbm, rope_t_hbm, y_ref, k_ref, v_ref,
                 x_v, g_v, rope_r, rope_t, wqkv, wgu, wod, a_s, q_s, s_s, m_s, l_s, o_s, om_s,
                 part, swap, fwd, from_l, from_r, load_sem, send_sem, recv_sem):
    tokens, width = x_v.shape
    blocks = tokens // ROWS
    half = ROWS // 2
    n_chip = n_tp // 2
    chunk = half // n_chip
    wh = width // 2
    qw = wq_hbm.shape[1]
    heads = qw // HEAD_DIM
    ff = wg_hbm.shape[1]
    me = lax.axis_index('tp')
    chip, core = me // 2, lax.rem(me, 2)
    partner = chip * 2 + 1 - core
    c_r = lax.rem(chip + 1, n_chip)
    c_l = lax.rem(chip + n_chip - 1, n_chip)
    c_o = lax.rem(chip + 2, n_chip)
    right = c_r * 2 + core
    left = c_l * 2 + core

    kv_col = pl.multiple_of(me * HEAD_DIM, HEAD_DIM)
    def x_load(t):
        rows = pl.ds(pl.multiple_of(t * ROWS, ROWS), ROWS)
        return pltpu.make_async_copy(x_hbm.at[rows], x_v.at[rows], load_sem.at[8 + 2 * (ff // TILE) + t])
    def load(i, src, dst):
        return pltpu.make_async_copy(src, dst, load_sem.at[i])
    small_loads = [
        load(0, g_hbm, g_v),
        load(1, rope_r_hbm, rope_r),
        load(2, rope_t_hbm, rope_t),
    ]
    qkv_loads = [
        load(3, wq_hbm, wqkv.at[:, pl.ds(0, qw)]),
        load(4, wk_hbm.at[:, pl.ds(kv_col, HEAD_DIM)], wqkv.at[:, pl.ds(qw, HEAD_DIM)]),
        load(5, wv_hbm.at[:, pl.ds(kv_col, HEAD_DIM)], wqkv.at[:, pl.ds(qw + HEAD_DIM, HEAD_DIM)]),
    ]
    ff_tiles = ff // TILE
    mlp_loads = []
    for j in range(ff_tiles):
        cols, up_cols = pl.ds(j * TILE, TILE), pl.ds(ff + j * TILE, TILE)
        mlp_loads.append([load(8 + 2 * j, wg_hbm.at[:, cols], wgu.at[:, cols]),
                          load(9 + 2 * j, wu_hbm.at[:, cols], wgu.at[:, up_cols])])
    out_loads = [
        load(6, wo_hbm, wod.at[pl.ds(0, qw)]),
        load(7, wd_hbm, wod.at[pl.ds(qw, ff)]),
    ]
    x_load(0).start()
    for cp in small_loads + qkv_loads + sum(mlp_loads, []) + out_loads:
        cp.start()
    for t in range(1, blocks):
        x_load(t).start()

    def first(t, copies):
        @pl.when(t == 0)
        def _():
            for cp in copies:
                cp.wait()

    barrier = pltpu.get_barrier_semaphore()
    for dev in (partner, left, right):
        pl.semaphore_signal(barrier, inc=1, device_id={'tp': dev}, device_id_type=MESH)
    pl.semaphore_wait(barrier, 3)

    def rows_of(t, c):
        return pl.ds(pl.multiple_of(t * ROWS + core * half + c * chunk, chunk), chunk)

    def slot(t):
        return pl.ds(pl.multiple_of(t * chunk, chunk), chunk)

    A, B = pl.ds(0, wh), pl.ds(wh, wh)

    def copy(kind, t):
        other = pl.ds(pl.multiple_of(t * ROWS + (1 - core) * half, half), half)
        src, dst, dev = {
            SWAP_A: lambda: (part.at[other, A], swap.at[pl.ds(pl.multiple_of(t * half, half), half), A], partner),
            SWAP_B: lambda: (part.at[other, B], swap.at[pl.ds(pl.multiple_of(t * half, half), half), B], partner),
            FWD_R: lambda: (part.at[rows_of(t, c_o), A], fwd.at[slot(t), A], right),
            OWN_R: lambda: (part.at[rows_of(t, c_r), B], from_l.at[slot(t), B], right),
            FWD_L: lambda: (part.at[rows_of(t, c_o), B], fwd.at[slot(t), B], left),
            OWN_L: lambda: (part.at[rows_of(t, c_l), A], from_r.at[slot(t), A], left),
            SUM_R: lambda: (part.at[rows_of(t, c_r), A], from_l.at[slot(t), A], right),
            SUM_L: lambda: (part.at[rows_of(t, c_l), B], from_r.at[slot(t), B], left),
            OUT_R: lambda: (y_ref.at[rows_of(t, chip)], y_ref.at[rows_of(t, chip)], right),
            OUT_L: lambda: (y_ref.at[rows_of(t, chip)], y_ref.at[rows_of(t, chip)], left),
            OUT_P: lambda: (y_ref.at[rows_of(t, chip)], y_ref.at[rows_of(t, chip)], partner),
            FAR_R: lambda: (y_ref.at[rows_of(t, c_l), A], y_ref.at[rows_of(t, c_l), A], right),
            FAR_L: lambda: (y_ref.at[rows_of(t, c_r), B], y_ref.at[rows_of(t, c_r), B], left),
            P_LEFT: lambda: (y_ref.at[rows_of(t, c_l)], y_ref.at[rows_of(t, c_l)], partner),
            P_RIGHT: lambda: (y_ref.at[rows_of(t, c_r)], y_ref.at[rows_of(t, c_r)], partner),
            P_FAR_A: lambda: (y_ref.at[rows_of(t, c_o), A], y_ref.at[rows_of(t, c_o), A], partner),
            P_FAR_B: lambda: (y_ref.at[rows_of(t, c_o), B], y_ref.at[rows_of(t, c_o), B], partner),
        }[kind]()
        return pltpu.make_async_remote_copy(
            src_ref=src, dst_ref=dst, send_sem=send_sem.at[kind, t], recv_sem=recv_sem.at[kind, t],
            device_id={'tp': dev}, device_id_type=MESH)

    scale = 1.0 / math.sqrt(HEAD_DIM) * math.log2(math.e)

    def project(t):
        x_load(t).wait()
        first(t, small_loads)
        step = 64
        gain = g_v[...].astype(F32).reshape(1, width)
        for i in range(ROWS // step):
            xf = x_v[pl.ds(pl.multiple_of(t * ROWS + i * step, step), step), :].astype(F32)
            inv = lax.rsqrt(jnp.mean(xf * xf, axis=-1, keepdims=True) + NORM_EPS)
            a_s[pl.ds(i * step, step), :] = (xf * inv * gain).astype(BF16)
        first(t, qkv_loads)
        a = a_s[...]
        c0, s0 = rope_t[0, pl.ds(t, 1), :], rope_t[1, pl.ds(t, 1), :]
        cos = rope_r[0] * c0 - rope_r[1] * s0
        sin = rope_r[1] * c0 + rope_r[0] * s0
        rot = lambda p: (p * cos + pltpu.roll(p, HEAD_DIM // 2, 1) * sin).astype(BF16)
        q = jnp.dot(a, wqkv[:, pl.ds(0, qw)], preferred_element_type=F32)
        kv = jnp.dot(a, wqkv[:, pl.ds(qw, 2 * HEAD_DIM)], preferred_element_type=F32)
        for h in range(heads):
            q_s[pl.ds(h * ROWS, ROWS), :] = rot(q[:, h * HEAD_DIM:(h + 1) * HEAD_DIM])
        rows = pl.ds(pl.multiple_of(t * ROWS, ROWS), ROWS)
        k_ref[rows, :] = rot(kv[:, :HEAD_DIM])
        v_ref[rows, :] = kv[:, HEAD_DIM:].astype(BF16)

    def lanes(op, s):
        acc = s[:, :128]
        for i in range(1, ROWS // 128):
            acc = op(acc, s[:, i * 128:(i + 1) * 128])
        return acc

    def keys(kb):
        return pl.ds(pl.multiple_of(kb * ROWS, ROWS), ROWS)

    def score(kb):
        return lax.dot_general(q_s[...], k_ref[keys(kb), :], (((1,), (1,)), ((), ())), preferred_element_type=F32)

    def attend_scores(t):
        s = score(t)
        shape = (heads, ROWS, ROWS)
        q_pos = lax.broadcasted_iota(jnp.int32, shape, 1).reshape(heads * ROWS, ROWS)
        k_pos = lax.broadcasted_iota(jnp.int32, shape, 2).reshape(heads * ROWS, ROWS)
        s = jnp.where(k_pos <= q_pos, s, -1e30)
        s_s[t] = s
        m_s[...] = lanes(jnp.maximum, s)

        def pass1(kb, _):
            s = score(kb)
            s_s[kb] = s
            m_s[...] = jnp.maximum(m_s[...], lanes(jnp.maximum, s))
            return 0
        lax.fori_loop(0, t, pass1, 0)
        m_s[...] = jnp.broadcast_to(jnp.max(m_s[...], axis=-1, keepdims=True) * scale, m_s.shape)
        l_s[...] = jnp.zeros_like(l_s)

        def pass2(kb, _):
            m = m_s[...]
            p = jnp.exp2(s_s[kb] * scale - jnp.concatenate([m] * (ROWS // 128), axis=1))
            s_s[kb] = p
            l_s[...] += lanes(jnp.add, p)
            return 0
        lax.fori_loop(0, t + 1, pass2, 0)

    def attend_values(t):
        l_s[...] = jnp.broadcast_to(1.0 / jnp.sum(l_s[...], axis=-1, keepdims=True), l_s.shape)
        o_s[...] = jnp.zeros_like(o_s)

        def pass3(kb, _):
            r = l_s[...]
            p = (s_s[kb] * jnp.concatenate([r] * (ROWS // 128), axis=1)).astype(BF16)
            o_s[...] += jnp.dot(p, v_ref[keys(kb), :], preferred_element_type=F32)
            return 0
        lax.fori_loop(0, t + 1, pass3, 0)
        for h in range(heads):
            om_s[:, pl.ds(h * HEAD_DIM, HEAD_DIM)] = o_s[pl.ds(h * ROWS, ROWS), :].astype(BF16)

    def mlp(t, j):
        first(t, mlp_loads[j])
        a = a_s[...]
        gate = jnp.dot(a, wgu[:, pl.ds(j * TILE, TILE)], preferred_element_type=F32)
        up = jnp.dot(a, wgu[:, pl.ds(ff + j * TILE, TILE)], preferred_element_type=F32)
        om_s[:, pl.ds(qw + j * TILE, TILE)] = (jax.nn.silu(gate) * up).astype(BF16)

    def out_half(t, which, kind):
        om = om_s[...]
        rows = pl.ds(pl.multiple_of(t * ROWS, ROWS), ROWS)
        tiles = width // TILE // 2
        for j in range(which * tiles, (which + 1) * tiles):
            cols = pl.ds(j * TILE, TILE)
            part[rows, cols] = jnp.dot(om, wod[:, cols], preferred_element_type=F32).astype(BF16)
        copy(kind, t).start()

    def chip_sum(t, cols, got, *sends):
        copy(got, t).wait_recv()
        for i in range(4):
            n = half // 4
            rows = pl.ds(pl.multiple_of(t * ROWS + core * half + i * n, n), n)
            other = swap[pl.ds(pl.multiple_of(t * half + i * n, n), n), cols].astype(F32)
            part[rows, cols] = (part[rows, cols].astype(F32) + other).astype(BF16)
        for kind in sends:
            copy(kind, t).start()

    def pass_on(t, cols, got, out, c):
        copy(got, t).wait_recv()
        rows = rows_of(t, c)
        part[rows, cols] = (part[rows, cols].astype(F32) + fwd[slot(t), cols].astype(F32)).astype(BF16)
        copy(out, t).start()

    def finish(t):
        for kind in (OWN_R, OWN_L, SUM_R, SUM_L):
            copy(kind, t).wait_recv()
        rows = rows_of(t, chip)
        total = (part[rows, :].astype(F32) + from_l[slot(t), :].astype(F32)) + from_r[slot(t), :].astype(F32)
        y_ref[rows, :] = (x_v[rows, :].astype(F32) + total).astype(BF16)
        for kind in (OUT_R, OUT_L, OUT_P):
            copy(kind, t).start()

    def spread(t):
        copy(OUT_R, t).wait_recv()
        copy(FAR_R, t).start()
        copy(P_LEFT, t).start()
        copy(OUT_L, t).wait_recv()
        copy(FAR_L, t).start()
        copy(P_RIGHT, t).start()

    def far(t):
        copy(FAR_R, t).wait_recv()
        copy(P_FAR_A, t).start()
        copy(FAR_L, t).wait_recv()
        copy(P_FAR_B, t).start()

    def close(t):
        for kind in (OUT_P, P_LEFT, P_RIGHT, P_FAR_A, P_FAR_B):
            copy(kind, t).wait_recv()
        for kind in range(N_KINDS):
            copy(kind, t).wait_send()

    stages = {
        'chip_sum_a': lambda t: chip_sum(t, A, SWAP_A, FWD_R, OWN_L),
        'chip_sum_b': lambda t: chip_sum(t, B, SWAP_B, FWD_L, OWN_R),
        'pass_on_a': lambda t: pass_on(t, A, FWD_R, SUM_R, c_r),
        'pass_on_b': lambda t: pass_on(t, B, FWD_L, SUM_L, c_l),
        'finish': finish, 'spread': spread, 'far': far, 'close': close,
    }

    def place(p, s):
        for name, lag in PLACES.get(p, ()):
            @pl.when(s >= lag)
            def _(name=name, lag=lag):
                stages[name](s - lag)

    def step(s, _):
        place('start', s)
        project(s)
        place('project', s)
        attend_scores(s)
        place('scores', s)
        attend_values(s)
        place('values', s)
        for j in range(ff_tiles):
            mlp(s, j)
            place('mlp%d' % j, s)
        first(s, out_loads)
        out_half(s, 0, SWAP_A)
        place('out0', s)
        out_half(s, 1, SWAP_B)
        place('out1', s)
        return 0

    lax.fori_loop(0, blocks, step, 0)
    for name, back in DRAIN:
        stages[name](blocks - 1 - back)


def store_kernel(y_ref, k_ref, v_ref, y_hbm, k_hbm, v_hbm, sem):
    n = y_ref.shape[0] // STORES
    copies = [pltpu.make_async_copy(y_ref.at[pl.ds(i * n, n)], y_hbm.at[pl.ds(i * n, n)], sem.at[2 + i])
              for i in range(STORES)]
    copies += [pltpu.make_async_copy(k_ref, k_hbm, sem.at[0]), pltpu.make_async_copy(v_ref, v_hbm, sem.at[1])]
    for cp in copies:
        cp.start()
    for cp in copies:
        cp.wait()


def solution(mesh):
    n_tp = mesh.shape['tp']

    def local_layer(x_in, g_norm, w_q, w_k, w_v, w_o, w_gate, w_up, w_down):
        tokens, width = x_in.shape
        blocks = tokens // ROWS
        qw, ff = w_q.shape[1], w_gate.shape[1]
        heads = qw // HEAD_DIM
        half = ROWS // 2
        chunk = half // (n_tp // 2)
        cos_r, sin_r, cos_t, sin_t = rope_constants(ROWS, blocks)
        consts = [jnp.asarray(np.stack([cos_r, sin_r])), jnp.asarray(np.stack([cos_t, sin_t]))]
        vm = lambda: pl.BlockSpec(memory_space=pltpu.VMEM)
        hbm = lambda: pl.BlockSpec(memory_space=pl.ANY)
        y_out, k_rot, v_proj = pl.pallas_call(
            functools.partial(layer_kernel, n_tp),
            out_shape=(pltpu.VMEM((tokens, width), BF16),
                       pltpu.VMEM((tokens, HEAD_DIM), BF16),
                       pltpu.VMEM((tokens, HEAD_DIM), BF16)),
            in_specs=[hbm()] * 11,
            out_specs=(vm(), vm(), vm()),
            scratch_shapes=[
                pltpu.VMEM((tokens, width), BF16),
                pltpu.VMEM((width,), BF16),
                pltpu.VMEM((2, ROWS, HEAD_DIM), F32),
                pltpu.VMEM((2, blocks, HEAD_DIM), F32),
                pltpu.VMEM((width, qw + 2 * HEAD_DIM), BF16),
                pltpu.VMEM((width, 2 * ff), BF16),
                pltpu.VMEM((qw + ff, width), BF16),
                pltpu.VMEM((ROWS, width), BF16),
                pltpu.VMEM((heads * ROWS, HEAD_DIM), BF16),
                pltpu.VMEM((tokens // ROWS, heads * ROWS, ROWS), F32),
                pltpu.VMEM((heads * ROWS, 128), F32),
                pltpu.VMEM((heads * ROWS, 128), F32),
                pltpu.VMEM((heads * ROWS, HEAD_DIM), F32),
                pltpu.VMEM((ROWS, qw + ff), BF16),
                pltpu.VMEM((tokens, width), BF16),
                pltpu.VMEM((tokens // 2, width), BF16),
                pltpu.VMEM((blocks * chunk, width), BF16),
                pltpu.VMEM((blocks * chunk, width), BF16),
                pltpu.VMEM((blocks * chunk, width), BF16),
                pltpu.SemaphoreType.DMA((8 + 2 * (ff // TILE) + blocks,)),
                pltpu.SemaphoreType.DMA((N_KINDS, blocks)),
                pltpu.SemaphoreType.DMA((N_KINDS, blocks)),
            ],
            compiler_params=pltpu.CompilerParams(
                collective_id=0, has_side_effects=True, vmem_limit_bytes=52 * 2**20),
            name='layer',
        )(x_in, g_norm, w_q, w_k, w_v, w_o, w_gate, w_up, w_down, *consts)
        y_out, k_rot, v_proj = pl.pallas_call(
            store_kernel,
            out_shape=tuple(jax.ShapeDtypeStruct(a.shape, BF16) for a in (y_out, k_rot, v_proj)),
            in_specs=[vm()] * 3, out_specs=(hbm(),) * 3,
            scratch_shapes=[pltpu.SemaphoreType.DMA((2 + STORES,))],
            compiler_params=pltpu.CompilerParams(vmem_limit_bytes=8 * 2**20),
            name='store',
        )(y_out, k_rot, v_proj)
        return y_out, k_rot.reshape(tokens, 1, HEAD_DIM), v_proj.reshape(tokens, 1, HEAD_DIM)

    return jax.shard_map(local_layer, mesh=mesh, in_specs=(P('dp', None), P(None), P(None, 'tp'), P(None, None), P(None, None), P('tp', None), P(None, 'tp'), P(None, 'tp'), P('tp', None)), out_specs=(P('dp', None), P('dp', 'tp', None), P('dp', 'tp', None)), check_vma=False)
```

```python
import functools
import math
import numpy as np
import jax
import jax.numpy as jnp
from jax import lax
from jax.experimental import pallas as pl
from jax.experimental.pallas import tpu as pltpu
from jax.sharding import PartitionSpec as P

HEAD_DIM = 128
ROPE_BASE = 500000.0
NORM_EPS = 1e-5
ROWS = 256
TILE = 256
STORES = 8
F32 = jnp.float32
BF16 = jnp.bfloat16
MESH = pl.DeviceIdType.MESH

(SWAP_A, SWAP_B, FWD_R, OWN_L, FWD_L, OWN_R, SUM_R, SUM_L, OUT_R, OUT_L, OUT_P, FAR_R, FAR_L,
 P_LEFT, P_RIGHT, P_FAR_A, P_FAR_B) = range(17)
R_SWAP_A, R_SWAP_B, R_FWD_R, R_FWD_L, R_FIN, R_OUT, R_FAR = range(7)
N_RECV = 7
ARRIVES = {SWAP_A: R_SWAP_A, SWAP_B: R_SWAP_B, FWD_R: R_FWD_R, FWD_L: R_FWD_L, OWN_L: R_FIN, OWN_R: R_FIN,
           SUM_R: R_FIN, SUM_L: R_FIN, OUT_R: R_OUT, OUT_L: R_OUT, FAR_R: R_FAR, FAR_L: R_FAR}
S_SWAP, S_LINK, S_PARTNER = range(3)

PLACES = {
    (1, 'project'): (('chip_sum_a', 0),),
    (1, 'values'): (('chip_sum_b', 0),),
    (1, 'out1'): (('pass_on_a', 0),),
    (2, 'start'): (('pass_on_b', 0),),
    (2, 'project'): (('chip_sum_a', 1),),
    (2, 'values'): (('chip_sum_b', 1),),
    (2, 'mlp1'): (('finish', 0),),
    (2, 'out1'): (('pass_on_a', 1),),
    (3, 'start'): (('pass_on_b', 1),),
    (3, 'project'): (('chip_sum_a', 2),),
    (3, 'values'): (('chip_sum_b', 2),),
    (3, 'mlp1'): (('finish', 1),),
    (3, 'out1'): (('pass_on_a', 2),),
    (4, 'start'): (('pass_on_b', 2),),
    (4, 'project'): (('spread', 0), ('chip_sum_a', 3),),
    (4, 'values'): (('chip_sum_b', 3),),
    (4, 'mlp1'): (('finish', 2),),
    (4, 'out1'): (('far', 0), ('pass_on_a', 3),),
    (5, 'start'): (('pass_on_b', 3),),
    (5, 'project'): (('spread', 1), ('chip_sum_a', 4),),
    (5, 'values'): (('chip_sum_b', 4),),
    (5, 'mlp1'): (('finish', 3),),
    (5, 'out1'): (('far', 1), ('pass_on_a', 4),),
}
DRAIN = (
    ('spread', 2), ('chip_sum_a', 5), ('chip_sum_b', 5), ('pass_on_b', 4),
    ('spread', 3), ('far', 2), ('pass_on_a', 5), ('pass_on_b', 5),
    ('finish', 4), ('far', 3), ('finish', 5), ('spread', 4),
    ('spread', 5), ('far', 4), ('far', 5),
)


def rope_constants(rows, blocks):
    inv_freq = ROPE_BASE ** (-np.arange(0, HEAD_DIM, 2, dtype=np.float64) / HEAD_DIM)
    def tables(positions):
        ang = positions[:, None] * inv_freq[None, :]
        cos, sin = np.cos(ang), np.sin(ang)
        return (np.concatenate([cos, cos], 1).astype(np.float32),
                np.concatenate([-sin, sin], 1).astype(np.float32))
    cos_r, sin_r = tables(np.arange(rows, dtype=np.float64))
    cos_t, sin_t = tables(np.arange(blocks, dtype=np.float64) * rows)
    return cos_r, sin_r, cos_t, sin_t


def layer_kernel(n_tp, x_hbm, g_hbm, wq_hbm, wk_hbm, wv_hbm, wo_hbm, wg_hbm, wu_hbm, wd_hbm,
                 rope_hbm, y_ref, k_ref, v_ref,
                 x_v, g_v, rope, wqkv, wgu, wod, a_s, q_s, s_s, m_s, l_s, o_s, om_s,
                 part, swap, fwd, from_l, from_r, load_sem, send_sem, recv_sem, done_sem):
    tokens, width = x_v.shape
    blocks = tokens // ROWS
    half = ROWS // 2
    n_chip = n_tp // 2
    chunk = half // n_chip
    wh = width // 2
    qw = wq_hbm.shape[1]
    heads = qw // HEAD_DIM
    ff = wg_hbm.shape[1]
    me = lax.axis_index('tp')
    chip, core = me // 2, lax.rem(me, 2)
    partner = chip * 2 + 1 - core
    c_r = lax.rem(chip + 1, n_chip)
    c_l = lax.rem(chip + n_chip - 1, n_chip)
    c_o = lax.rem(chip + 2, n_chip)
    right = c_r * 2 + core
    left = c_l * 2 + core

    A, B = pl.ds(0, wh), pl.ds(wh, wh)

    kv_col = pl.multiple_of(me * HEAD_DIM, HEAD_DIM)
    def x_load(t):
        rows = pl.ds(pl.multiple_of(t * ROWS, ROWS), ROWS)
        return pltpu.make_async_copy(x_hbm.at[rows], x_v.at[rows], load_sem.at[5 + ff // TILE + t])
    def load(i, src, dst):
        return pltpu.make_async_copy(src, dst, load_sem.at[i])
    ff_tiles = ff // TILE
    L_SMALL, L_QKV, L_OUT, L_MLP, L_X = 0, 2, 3, 5, 5 + ff_tiles
    small_loads = [load(L_SMALL, g_hbm, g_v), load(L_SMALL + 1, rope_hbm, rope)]
    qkv_loads = [
        load(L_QKV, wq_hbm, wqkv.at[:, pl.ds(0, qw)]),
        load(L_QKV, wk_hbm.at[:, pl.ds(kv_col, HEAD_DIM)], wqkv.at[:, pl.ds(qw, HEAD_DIM)]),
        load(L_QKV, wv_hbm.at[:, pl.ds(kv_col, HEAD_DIM)], wqkv.at[:, pl.ds(qw + HEAD_DIM, HEAD_DIM)]),
    ]
    mlp_loads = []
    for j in range(ff_tiles):
        cols, up_cols = pl.ds(j * TILE, TILE), pl.ds(ff + j * TILE, TILE)
        mlp_loads += [load(L_MLP + j, wg_hbm.at[:, cols], wgu.at[:, cols]),
                      load(L_MLP + j, wu_hbm.at[:, cols], wgu.at[:, up_cols])]
    out_loads = []
    for i, cols in enumerate((A, B)):
        out_loads += [load(L_OUT + i, wo_hbm.at[:, cols], wod.at[pl.ds(0, qw), cols]),
                      load(L_OUT + i, wd_hbm.at[:, cols], wod.at[pl.ds(qw, ff), cols])]
    x_load(0).start()
    for cp in small_loads + qkv_loads + mlp_loads + out_loads:
        cp.start()
    for t in range(1, blocks):
        x_load(t).start()

    def loaded(t, sem, ref):
        if t == 0:
            load(sem, ref, ref).wait()

    barrier = pltpu.get_barrier_semaphore()
    for dev in (partner, left, right):
        pl.semaphore_signal(barrier, inc=1, device_id={'tp': dev}, device_id_type=MESH)
    def rows_of(t, c):
        return pl.ds(pl.multiple_of(t * ROWS + core * half + c * chunk, chunk), chunk)

    def slot(t):
        return pl.ds(pl.multiple_of(t * chunk, chunk), chunk)

    def copy(kind, t):
        other = pl.ds(pl.multiple_of(t * ROWS + (1 - core) * half, half), half)
        src, dst, dev = {
            SWAP_A: lambda: (part.at[other, A], swap.at[pl.ds(pl.multiple_of(t * half, half), half), A], partner),
            SWAP_B: lambda: (part.at[other, B], swap.at[pl.ds(pl.multiple_of(t * half, half), half), B], partner),
            FWD_R: lambda: (part.at[rows_of(t, c_o), A], fwd.at[slot(t), A], right),
            OWN_R: lambda: (part.at[rows_of(t, c_r), B], from_l.at[slot(t), B], right),
            FWD_L: lambda: (part.at[rows_of(t, c_o), B], fwd.at[slot(t), B], left),
            OWN_L: lambda: (part.at[rows_of(t, c_l), A], from_r.at[slot(t), A], left),
            SUM_R: lambda: (part.at[rows_of(t, c_r), A], from_l.at[slot(t), A], right),
            SUM_L: lambda: (part.at[rows_of(t, c_l), B], from_r.at[slot(t), B], left),
            OUT_R: lambda: (y_ref.at[rows_of(t, chip)], y_ref.at[rows_of(t, chip)], right),
            OUT_L: lambda: (y_ref.at[rows_of(t, chip)], y_ref.at[rows_of(t, chip)], left),
            OUT_P: lambda: (y_ref.at[rows_of(t, chip)], y_ref.at[rows_of(t, chip)], partner),
            FAR_R: lambda: (y_ref.at[rows_of(t, c_l), A], y_ref.at[rows_of(t, c_l), A], right),
            FAR_L: lambda: (y_ref.at[rows_of(t, c_r), B], y_ref.at[rows_of(t, c_r), B], left),
            P_LEFT: lambda: (y_ref.at[rows_of(t, c_l)], y_ref.at[rows_of(t, c_l)], partner),
            P_RIGHT: lambda: (y_ref.at[rows_of(t, c_r)], y_ref.at[rows_of(t, c_r)], partner),
            P_FAR_A: lambda: (y_ref.at[rows_of(t, c_o), A], y_ref.at[rows_of(t, c_o), A], partner),
            P_FAR_B: lambda: (y_ref.at[rows_of(t, c_o), B], y_ref.at[rows_of(t, c_o), B], partner),
        }[kind]()
        leaves = S_SWAP if kind in (SWAP_A, SWAP_B) else S_LINK if kind in ARRIVES else S_PARTNER
        return pltpu.make_async_remote_copy(
            src_ref=src, dst_ref=dst, send_sem=send_sem.at[leaves],
            recv_sem=recv_sem.at[ARRIVES[kind], t] if kind in ARRIVES else done_sem.at[0],
            device_id={'tp': dev}, device_id_type=MESH)

    def take(sem, rows):
        ref = y_ref.at[pl.ds(0, rows)]
        pltpu.make_async_copy(ref, ref, sem).wait()

    scale = 1.0 / math.sqrt(HEAD_DIM) * math.log2(math.e)

    def project(t):
        x_load(t).wait()
        if t == 0:
            for cp in small_loads:
                cp.wait()
        step = 64
        gain = g_v[...].astype(F32).reshape(1, width)
        for i in range(ROWS // step):
            xf = x_v[pl.ds(pl.multiple_of(t * ROWS + i * step, step), step), :].astype(F32)
            inv = lax.rsqrt(jnp.mean(xf * xf, axis=-1, keepdims=True) + NORM_EPS)
            a_s[pl.ds(i * step, step), :] = (xf * inv * gain).astype(BF16)
        loaded(t, L_QKV, wqkv)
        a = a_s[...]
        c0, s0 = rope[0, pl.ds(ROWS + t, 1), :], rope[1, pl.ds(ROWS + t, 1), :]
        cos_r, sin_r = rope[0, :ROWS, :], rope[1, :ROWS, :]
        cos = cos_r * c0 - sin_r * s0
        sin = sin_r * c0 + cos_r * s0
        rot = lambda p: (p * cos + pltpu.roll(p, HEAD_DIM // 2, 1) * sin).astype(BF16)
        q = jnp.dot(a, wqkv[:, pl.ds(0, qw)], preferred_element_type=F32)
        kv = jnp.dot(a, wqkv[:, pl.ds(qw, 2 * HEAD_DIM)], preferred_element_type=F32)
        for h in range(heads):
            q_s[pl.ds(h * ROWS, ROWS), :] = rot(q[:, h * HEAD_DIM:(h + 1) * HEAD_DIM])
        rows = pl.ds(pl.multiple_of(t * ROWS, ROWS), ROWS)
        k_ref[rows, :] = rot(kv[:, :HEAD_DIM])
        v_ref[rows, :] = kv[:, HEAD_DIM:].astype(BF16)

    def lanes(op, s):
        acc = s[:, :128]
        for i in range(1, ROWS // 128):
            acc = op(acc, s[:, i * 128:(i + 1) * 128])
        return acc

    def keys(kb):
        return pl.ds(pl.multiple_of(kb * ROWS, ROWS), ROWS)

    def score(kb):
        return lax.dot_general(q_s[...], k_ref[keys(kb), :], (((1,), (1,)), ((), ())), preferred_element_type=F32)

    def attend_scores(t):
        s = score(t)
        shape = (heads, ROWS, ROWS)
        q_pos = lax.broadcasted_iota(jnp.int32, shape, 1).reshape(heads * ROWS, ROWS)
        k_pos = lax.broadcasted_iota(jnp.int32, shape, 2).reshape(heads * ROWS, ROWS)
        s = jnp.where(k_pos <= q_pos, s, -1e30)
        s_s[t] = s
        m_s[...] = lanes(jnp.maximum, s)

        for kb in range(t):
            s = score(kb)
            s_s[kb] = s
            m_s[...] = jnp.maximum(m_s[...], lanes(jnp.maximum, s))
        m_s[...] = jnp.broadcast_to(jnp.max(m_s[...], axis=-1, keepdims=True) * scale, m_s.shape)
        l_s[...] = jnp.zeros_like(l_s)

        for kb in range(t + 1):
            m = m_s[...]
            p = jnp.exp2(s_s[kb] * scale - jnp.concatenate([m] * (ROWS // 128), axis=1))
            s_s[kb] = p
            l_s[...] += lanes(jnp.add, p)

    def attend_values(t):
        l_s[...] = jnp.broadcast_to(1.0 / jnp.sum(l_s[...], axis=-1, keepdims=True), l_s.shape)
        o_s[...] = jnp.zeros_like(o_s)

        for kb in range(t + 1):
            r = l_s[...]
            p = (s_s[kb] * jnp.concatenate([r] * (ROWS // 128), axis=1)).astype(BF16)
            o_s[...] += jnp.dot(p, v_ref[keys(kb), :], preferred_element_type=F32)
        for h in range(heads):
            om_s[:, pl.ds(h * HEAD_DIM, HEAD_DIM)] = o_s[pl.ds(h * ROWS, ROWS), :].astype(BF16)

    def mlp(t, j):
        loaded(t, L_MLP + j, wgu.at[:, pl.ds(0, 2 * TILE)])
        a = a_s[...]
        gate = jnp.dot(a, wgu[:, pl.ds(j * TILE, TILE)], preferred_element_type=F32)
        up = jnp.dot(a, wgu[:, pl.ds(ff + j * TILE, TILE)], preferred_element_type=F32)
        om_s[:, pl.ds(qw + j * TILE, TILE)] = (jax.nn.silu(gate) * up).astype(BF16)

    def out_half(t, which, kind):
        loaded(t, L_OUT + which, wod.at[:, A])
        om = om_s[...]
        rows = pl.ds(pl.multiple_of(t * ROWS, ROWS), ROWS)
        tiles = width // TILE // 2
        for j in range(which * tiles, (which + 1) * tiles):
            cols = pl.ds(j * TILE, TILE)
            part[rows, cols] = jnp.dot(om, wod[:, cols], preferred_element_type=F32).astype(BF16)
        copy(kind, t).start()

    def chip_sum(t, cols, got, *sends):
        copy(got, t).wait_recv()
        for i in range(4):
            n = half // 4
            rows = pl.ds(pl.multiple_of(t * ROWS + core * half + i * n, n), n)
            other = swap[pl.ds(pl.multiple_of(t * half + i * n, n), n), cols].astype(F32)
            part[rows, cols] = (part[rows, cols].astype(F32) + other).astype(BF16)
        for kind in sends:
            copy(kind, t).start()

    def pass_on(t, cols, got, out, c):
        copy(got, t).wait_recv()
        rows = rows_of(t, c)
        part[rows, cols] = (part[rows, cols].astype(F32) + fwd[slot(t), cols].astype(F32)).astype(BF16)
        copy(out, t).start()

    def finish(t):
        take(recv_sem.at[R_FIN, t], 2 * chunk)
        rows = rows_of(t, chip)
        total = (part[rows, :].astype(F32) + from_l[slot(t), :].astype(F32)) + from_r[slot(t), :].astype(F32)
        y_ref[rows, :] = (x_v[rows, :].astype(F32) + total).astype(BF16)
        for kind in (OUT_R, OUT_L, OUT_P):
            copy(kind, t).start()

    def spread(t):
        take(recv_sem.at[R_OUT, t], 2 * chunk)
        for kind in (FAR_R, FAR_L, P_LEFT, P_RIGHT):
            copy(kind, t).start()

    def far(t):
        take(recv_sem.at[R_FAR, t], chunk)
        for kind in (P_FAR_A, P_FAR_B):
            copy(kind, t).start()

    stages = {
        'chip_sum_a': lambda t: chip_sum(t, A, SWAP_A, FWD_R, OWN_L),
        'chip_sum_b': lambda t: chip_sum(t, B, SWAP_B, FWD_L, OWN_R),
        'pass_on_a': lambda t: pass_on(t, A, FWD_R, SUM_R, c_r),
        'pass_on_b': lambda t: pass_on(t, B, FWD_L, SUM_L, c_l),
        'finish': finish, 'spread': spread, 'far': far,
    }

    def place(p, s):
        for name, t in PLACES.get((s, p), ()):
            stages[name](t)

    def step(s):
        place('start', s)
        project(s)
        place('project', s)
        attend_scores(s)
        place('scores', s)
        attend_values(s)
        place('values', s)
        for j in range(ff_tiles):
            mlp(s, j)
            place('mlp%d' % j, s)
        if s == 0:
            pl.semaphore_wait(barrier, 3)
        out_half(s, 0, SWAP_A)
        place('out0', s)
        out_half(s, 1, SWAP_B)
        place('out1', s)

    for s in range(blocks):
        step(s)
    for name, t in DRAIN:
        stages[name](t)
    take(done_sem.at[0], tokens // 2)
    take(send_sem.at[S_SWAP], tokens // 2)
    take(send_sem.at[S_LINK], tokens * 3 // 4)
    take(send_sem.at[S_PARTNER], tokens // 2)


def store_kernel(y_ref, k_ref, v_ref, y_hbm, k_hbm, v_hbm, sem):
    n = y_ref.shape[0] // STORES
    copies = [pltpu.make_async_copy(y_ref.at[pl.ds(i * n, n)], y_hbm.at[pl.ds(i * n, n)], sem.at[2 + i])
              for i in range(STORES)]
    copies += [pltpu.make_async_copy(k_ref, k_hbm, sem.at[0]), pltpu.make_async_copy(v_ref, v_hbm, sem.at[1])]
    for cp in copies:
        cp.start()
    for cp in copies:
        cp.wait()


def solution(mesh):
    n_tp = mesh.shape['tp']

    def local_layer(x_in, g_norm, w_q, w_k, w_v, w_o, w_gate, w_up, w_down):
        tokens, width = x_in.shape
        blocks = tokens // ROWS
        qw, ff = w_q.shape[1], w_gate.shape[1]
        heads = qw // HEAD_DIM
        half = ROWS // 2
        chunk = half // (n_tp // 2)
        cos_r, sin_r, cos_t, sin_t = rope_constants(ROWS, blocks)
        rope = np.stack([np.concatenate([cos_r, cos_t]), np.concatenate([sin_r, sin_t])])
        rope = jnp.asarray(np.pad(rope, ((0, 0), (0, -blocks % 8), (0, 0))))
        vm = lambda: pl.BlockSpec(memory_space=pltpu.VMEM)
        hbm = lambda: pl.BlockSpec(memory_space=pl.ANY)
        y_out, k_rot, v_proj = pl.pallas_call(
            functools.partial(layer_kernel, n_tp),
            out_shape=(pltpu.VMEM((tokens, width), BF16),
                       pltpu.VMEM((tokens, HEAD_DIM), BF16),
                       pltpu.VMEM((tokens, HEAD_DIM), BF16)),
            in_specs=[hbm()] * 10,
            out_specs=(vm(), vm(), vm()),
            scratch_shapes=[
                pltpu.VMEM((tokens, width), BF16),
                pltpu.VMEM((width,), BF16),
                pltpu.VMEM(rope.shape, F32),
                pltpu.VMEM((width, qw + 2 * HEAD_DIM), BF16),
                pltpu.VMEM((width, 2 * ff), BF16),
                pltpu.VMEM((qw + ff, width), BF16),
                pltpu.VMEM((ROWS, width), BF16),
                pltpu.VMEM((heads * ROWS, HEAD_DIM), BF16),
                pltpu.VMEM((tokens // ROWS, heads * ROWS, ROWS), F32),
                pltpu.VMEM((heads * ROWS, 128), F32),
                pltpu.VMEM((heads * ROWS, 128), F32),
                pltpu.VMEM((heads * ROWS, HEAD_DIM), F32),
                pltpu.VMEM((ROWS, qw + ff), BF16),
                pltpu.VMEM((tokens, width), BF16),
                pltpu.VMEM((tokens // 2, width), BF16),
                pltpu.VMEM((blocks * chunk, width), BF16),
                pltpu.VMEM((blocks * chunk, width), BF16),
                pltpu.VMEM((blocks * chunk, width), BF16),
                pltpu.SemaphoreType.DMA((5 + ff // TILE + blocks,)),
                pltpu.SemaphoreType.DMA((3,)),
                pltpu.SemaphoreType.DMA((N_RECV, blocks)),
                pltpu.SemaphoreType.DMA((1,)),
            ],
            compiler_params=pltpu.CompilerParams(
                collective_id=0, has_side_effects=True, vmem_limit_bytes=52 * 2**20),
            name='layer',
        )(x_in, g_norm, w_q, w_k, w_v, w_o, w_gate, w_up, w_down, rope)
        y_out, k_rot, v_proj = pl.pallas_call(
            store_kernel,
            out_shape=tuple(jax.ShapeDtypeStruct(a.shape, BF16) for a in (y_out, k_rot, v_proj)),
            in_specs=[vm()] * 3, out_specs=(hbm(),) * 3,
            scratch_shapes=[pltpu.SemaphoreType.DMA((2 + STORES,))],
            compiler_params=pltpu.CompilerParams(vmem_limit_bytes=8 * 2**20),
            name='store',
        )(y_out, k_rot, v_proj)
        return y_out, k_rot.reshape(tokens, 1, HEAD_DIM), v_proj.reshape(tokens, 1, HEAD_DIM)

    return jax.shard_map(local_layer, mesh=mesh, in_specs=(P('dp', None), P(None), P(None, 'tp'), P(None, None), P(None, None), P('tp', None), P(None, 'tp'), P(None, 'tp'), P('tp', None)), out_specs=(P('dp', None), P('dp', 'tp', None), P('dp', 'tp', None)), check_vma=False)
```

```python
import functools
import math
import numpy as np
import jax
import jax.numpy as jnp
from jax import lax
from jax.experimental import pallas as pl
from jax.experimental.pallas import tpu as pltpu
from jax.sharding import PartitionSpec as P

HEAD_DIM = 128
ROPE_BASE = 500000.0
NORM_EPS = 1e-5
ROWS = 256
TILE = 256
STORES = 8
F32 = jnp.float32
BF16 = jnp.bfloat16
MESH = pl.DeviceIdType.MESH

(SWAP_A, SWAP_B, FWD_R, OWN_L, FWD_L, OWN_R, SUM_R, SUM_L, OUT_R, OUT_L, OUT_P, FAR_R, FAR_L,
 P_LEFT, P_RIGHT, P_FAR_A, P_FAR_B) = range(17)
R_SWAP_A, R_SWAP_B, R_FWD_R, R_FWD_L, R_FIN, R_OUT, R_FAR = range(7)
N_RECV = 7
ARRIVES = {SWAP_A: R_SWAP_A, SWAP_B: R_SWAP_B, FWD_R: R_FWD_R, FWD_L: R_FWD_L, OWN_L: R_FIN, OWN_R: R_FIN,
           SUM_R: R_FIN, SUM_L: R_FIN, OUT_R: R_OUT, OUT_L: R_OUT, FAR_R: R_FAR, FAR_L: R_FAR}
S_SWAP, S_LINK, S_PARTNER = range(3)

PLACES = {
    (1, 'project'): (('chip_sum_a', 0), ('chip_sum_b', 0),),
    (1, 'out1'): (('pass_on_a', 0), ('pass_on_b', 0), ('chip_sum_a', 1),),
    (2, 'project'): (('chip_sum_b', 1),),
    (2, 'mlp2'): (('finish', 0),),
    (2, 'out1'): (('pass_on_a', 1), ('pass_on_b', 1), ('chip_sum_b', 2),),
    (3, 'project'): (('chip_sum_a', 2),),
    (3, 'mlp2'): (('spread', 0), ('finish', 1), ('pass_on_b', 2),),
    (3, 'out1'): (('pass_on_a', 2),),
    (4, 'project'): (('chip_sum_a', 3), ('chip_sum_b', 3),),
    (4, 'out1'): (('finish', 2), ('chip_sum_a', 4),),
    (5, 'project'): (('spread', 1),),
    (5, 'mlp2'): (('spread', 2), ('chip_sum_b', 4),),
    (5, 'out1'): (('chip_sum_a', 5), ('chip_sum_b', 5),),
}
DRAIN = (
    ('pass_on_a', 3), ('pass_on_a', 4), ('pass_on_b', 3), ('far', 0),
    ('far', 1), ('far', 2), ('pass_on_b', 4), ('pass_on_a', 5),
    ('pass_on_b', 5), ('finish', 3), ('finish', 4), ('finish', 5),
    ('spread', 3), ('spread', 4), ('spread', 5), ('far', 3),
    ('far', 4), ('far', 5),
)


def rope_constants(rows, blocks):
    inv_freq = ROPE_BASE ** (-np.arange(0, HEAD_DIM, 2, dtype=np.float64) / HEAD_DIM)
    def tables(positions):
        ang = positions[:, None] * inv_freq[None, :]
        cos, sin = np.cos(ang), np.sin(ang)
        return (np.concatenate([cos, cos], 1).astype(np.float32),
                np.concatenate([-sin, sin], 1).astype(np.float32))
    cos_r, sin_r = tables(np.arange(rows, dtype=np.float64))
    cos_t, sin_t = tables(np.arange(blocks, dtype=np.float64) * rows)
    return cos_r, sin_r, cos_t, sin_t


def layer_kernel(n_tp, x_hbm, g_hbm, wq_hbm, wk_hbm, wv_hbm, wo_hbm, wg_hbm, wu_hbm, wd_hbm,
                 rope_hbm, y_ref, k_ref, v_ref,
                 x_v, g_v, rope, wqkv, wgu, wod, a_s, q_s, s_s, m_s, l_s, o_s, om_s,
                 part, swap, fwd, from_l, from_r, load_sem, send_sem, recv_sem, done_sem):
    tokens, width = x_v.shape
    blocks = tokens // ROWS
    half = ROWS // 2
    n_chip = n_tp // 2
    chunk = half // n_chip
    wh = width // 2
    qw = wq_hbm.shape[1]
    heads = qw // HEAD_DIM
    ff = wg_hbm.shape[1]
    me = lax.axis_index('tp')
    chip, core = me // 2, lax.rem(me, 2)
    partner = chip * 2 + 1 - core
    c_r = lax.rem(chip + 1, n_chip)
    c_l = lax.rem(chip + n_chip - 1, n_chip)
    c_o = lax.rem(chip + 2, n_chip)
    right = c_r * 2 + core
    left = c_l * 2 + core

    A, B = pl.ds(0, wh), pl.ds(wh, wh)

    kv_col = pl.multiple_of(me * HEAD_DIM, HEAD_DIM)
    def x_load(t):
        rows = pl.ds(pl.multiple_of(t * ROWS, ROWS), ROWS)
        return pltpu.make_async_copy(x_hbm.at[rows], x_v.at[rows], load_sem.at[5 + t])
    def load(i, src, dst):
        return pltpu.make_async_copy(src, dst, load_sem.at[i])
    ff_tiles = ff // TILE
    L_SMALL, L_QKV, L_MLP, L_OUT = 0, 2, 3, 4
    small_loads = [load(L_SMALL, g_hbm, g_v), load(L_SMALL + 1, rope_hbm, rope)]
    qkv_loads = [
        load(L_QKV, wq_hbm, wqkv.at[:, pl.ds(0, qw)]),
        load(L_QKV, wk_hbm.at[:, pl.ds(kv_col, HEAD_DIM)], wqkv.at[:, pl.ds(qw, HEAD_DIM)]),
        load(L_QKV, wv_hbm.at[:, pl.ds(kv_col, HEAD_DIM)], wqkv.at[:, pl.ds(qw + HEAD_DIM, HEAD_DIM)]),
    ]
    mlp_loads = [load(L_MLP, wg_hbm, wgu.at[:, pl.ds(0, ff)]), load(L_MLP, wu_hbm, wgu.at[:, pl.ds(ff, ff)])]
    out_loads = [load(L_OUT, wo_hbm, wod.at[pl.ds(0, qw)]), load(L_OUT, wd_hbm, wod.at[pl.ds(qw, ff)])]
    x_load(0).start()
    for cp in small_loads + qkv_loads + mlp_loads + out_loads:
        cp.start()
    for t in range(1, blocks):
        x_load(t).start()

    def loaded(t, sem, ref):
        if t == 0:
            load(sem, ref, ref).wait()

    barrier = pltpu.get_barrier_semaphore()
    for dev in (partner, left, right):
        pl.semaphore_signal(barrier, inc=1, device_id={'tp': dev}, device_id_type=MESH)
    def rows_of(t, c):
        return pl.ds(pl.multiple_of(t * ROWS + core * half + c * chunk, chunk), chunk)

    def slot(t):
        return pl.ds(pl.multiple_of(t * chunk, chunk), chunk)

    def copy(kind, t):
        other = pl.ds(pl.multiple_of(t * ROWS + (1 - core) * half, half), half)
        src, dst, dev = {
            SWAP_A: lambda: (part.at[other, A], swap.at[pl.ds(pl.multiple_of(t * half, half), half), A], partner),
            SWAP_B: lambda: (part.at[other, B], swap.at[pl.ds(pl.multiple_of(t * half, half), half), B], partner),
            FWD_R: lambda: (part.at[rows_of(t, c_o), A], fwd.at[slot(t), A], right),
            OWN_R: lambda: (part.at[rows_of(t, c_r), B], from_l.at[slot(t), B], right),
            FWD_L: lambda: (part.at[rows_of(t, c_o), B], fwd.at[slot(t), B], left),
            OWN_L: lambda: (part.at[rows_of(t, c_l), A], from_r.at[slot(t), A], left),
            SUM_R: lambda: (part.at[rows_of(t, c_r), A], from_l.at[slot(t), A], right),
            SUM_L: lambda: (part.at[rows_of(t, c_l), B], from_r.at[slot(t), B], left),
            OUT_R: lambda: (y_ref.at[rows_of(t, chip)], y_ref.at[rows_of(t, chip)], right),
            OUT_L: lambda: (y_ref.at[rows_of(t, chip)], y_ref.at[rows_of(t, chip)], left),
            OUT_P: lambda: (y_ref.at[rows_of(t, chip)], y_ref.at[rows_of(t, chip)], partner),
            FAR_R: lambda: (y_ref.at[rows_of(t, c_l), A], y_ref.at[rows_of(t, c_l), A], right),
            FAR_L: lambda: (y_ref.at[rows_of(t, c_r), B], y_ref.at[rows_of(t, c_r), B], left),
            P_LEFT: lambda: (y_ref.at[rows_of(t, c_l)], y_ref.at[rows_of(t, c_l)], partner),
            P_RIGHT: lambda: (y_ref.at[rows_of(t, c_r)], y_ref.at[rows_of(t, c_r)], partner),
            P_FAR_A: lambda: (y_ref.at[rows_of(t, c_o), A], y_ref.at[rows_of(t, c_o), A], partner),
            P_FAR_B: lambda: (y_ref.at[rows_of(t, c_o), B], y_ref.at[rows_of(t, c_o), B], partner),
        }[kind]()
        leaves = S_SWAP if kind in (SWAP_A, SWAP_B) else S_LINK if kind in ARRIVES else S_PARTNER
        return pltpu.make_async_remote_copy(
            src_ref=src, dst_ref=dst, send_sem=send_sem.at[leaves],
            recv_sem=recv_sem.at[ARRIVES[kind], t] if kind in ARRIVES else done_sem.at[0],
            device_id={'tp': dev}, device_id_type=MESH)

    def take(sem, rows):
        ref = y_ref.at[pl.ds(0, rows)]
        pltpu.make_async_copy(ref, ref, sem).wait()

    scale = 1.0 / math.sqrt(HEAD_DIM) * math.log2(math.e)

    def project(t):
        if t == 0:
            for cp in small_loads:
                cp.wait()
        x_load(t).wait()
        step = 64
        gain = g_v[...].astype(F32).reshape(1, width)
        for i in range(ROWS // step):
            xf = x_v[pl.ds(pl.multiple_of(t * ROWS + i * step, step), step), :].astype(F32)
            inv = lax.rsqrt(jnp.mean(xf * xf, axis=-1, keepdims=True) + NORM_EPS)
            a_s[pl.ds(i * step, step), :] = (xf * inv * gain).astype(BF16)
        loaded(t, L_QKV, wqkv)
        a = a_s[...]
        c0, s0 = rope[0, pl.ds(ROWS + t, 1), :], rope[1, pl.ds(ROWS + t, 1), :]
        cos_r, sin_r = rope[0, :ROWS, :], rope[1, :ROWS, :]
        cos = cos_r * c0 - sin_r * s0
        sin = sin_r * c0 + cos_r * s0
        rot = lambda p: (p * cos + pltpu.roll(p, HEAD_DIM // 2, 1) * sin).astype(BF16)
        q = jnp.dot(a, wqkv[:, pl.ds(0, qw)], preferred_element_type=F32)
        kv = jnp.dot(a, wqkv[:, pl.ds(qw, 2 * HEAD_DIM)], preferred_element_type=F32)
        for h in range(heads):
            q_s[pl.ds(h * ROWS, ROWS), :] = rot(q[:, h * HEAD_DIM:(h + 1) * HEAD_DIM])
        rows = pl.ds(pl.multiple_of(t * ROWS, ROWS), ROWS)
        k_ref[rows, :] = rot(kv[:, :HEAD_DIM])
        v_ref[rows, :] = kv[:, HEAD_DIM:].astype(BF16)

    def lanes(op, s):
        acc = s[:, :128]
        for i in range(1, ROWS // 128):
            acc = op(acc, s[:, i * 128:(i + 1) * 128])
        return acc

    def keys(kb):
        return pl.ds(pl.multiple_of(kb * ROWS, ROWS), ROWS)

    def score(kb):
        return lax.dot_general(q_s[...], k_ref[keys(kb), :], (((1,), (1,)), ((), ())), preferred_element_type=F32)

    def attend_scores(t):
        s = score(t)
        shape = (heads, ROWS, ROWS)
        q_pos = lax.broadcasted_iota(jnp.int32, shape, 1).reshape(heads * ROWS, ROWS)
        k_pos = lax.broadcasted_iota(jnp.int32, shape, 2).reshape(heads * ROWS, ROWS)
        s = jnp.where(k_pos <= q_pos, s, -1e30)
        s_s[t] = s
        m_s[...] = lanes(jnp.maximum, s)

        for kb in range(t):
            s = score(kb)
            s_s[kb] = s
            m_s[...] = jnp.maximum(m_s[...], lanes(jnp.maximum, s))
        m_s[...] = jnp.broadcast_to(jnp.max(m_s[...], axis=-1, keepdims=True) * scale, m_s.shape)
        l_s[...] = jnp.zeros_like(l_s)

        for kb in range(t + 1):
            m = m_s[...]
            p = jnp.exp2(s_s[kb] * scale - jnp.concatenate([m] * (ROWS // 128), axis=1))
            s_s[kb] = p
            l_s[...] += lanes(jnp.add, p)

    def attend_values(t):
        l_s[...] = jnp.broadcast_to(1.0 / jnp.sum(l_s[...], axis=-1, keepdims=True), l_s.shape)
        o_s[...] = jnp.zeros_like(o_s)

        for kb in range(t + 1):
            r = l_s[...]
            p = (s_s[kb] * jnp.concatenate([r] * (ROWS // 128), axis=1)).astype(BF16)
            o_s[...] += jnp.dot(p, v_ref[keys(kb), :], preferred_element_type=F32)
        for h in range(heads):
            om_s[:, pl.ds(h * HEAD_DIM, HEAD_DIM)] = o_s[pl.ds(h * ROWS, ROWS), :].astype(BF16)

    def mlp(t, j):
        if j == 0:
            loaded(t, L_MLP, wgu)
        a = a_s[...]
        gate = jnp.dot(a, wgu[:, pl.ds(j * TILE, TILE)], preferred_element_type=F32)
        up = jnp.dot(a, wgu[:, pl.ds(ff + j * TILE, TILE)], preferred_element_type=F32)
        om_s[:, pl.ds(qw + j * TILE, TILE)] = (jax.nn.silu(gate) * up).astype(BF16)

    def out_half(t, which, kind):
        if which == 0:
            loaded(t, L_OUT, wod)
        om = om_s[...]
        rows = pl.ds(pl.multiple_of(t * ROWS, ROWS), ROWS)
        tiles = width // TILE // 2
        for j in range(which * tiles, (which + 1) * tiles):
            cols = pl.ds(j * TILE, TILE)
            part[rows, cols] = jnp.dot(om, wod[:, cols], preferred_element_type=F32).astype(BF16)
        copy(kind, t).start()

    def chip_sum(t, cols, got, *sends):
        copy(got, t).wait_recv()
        for i in range(4):
            n = half // 4
            rows = pl.ds(pl.multiple_of(t * ROWS + core * half + i * n, n), n)
            other = swap[pl.ds(pl.multiple_of(t * half + i * n, n), n), cols].astype(F32)
            part[rows, cols] = (part[rows, cols].astype(F32) + other).astype(BF16)
        for kind in sends:
            copy(kind, t).start()

    def pass_on(t, cols, got, out, c):
        copy(got, t).wait_recv()
        rows = rows_of(t, c)
        part[rows, cols] = (part[rows, cols].astype(F32) + fwd[slot(t), cols].astype(F32)).astype(BF16)
        copy(out, t).start()

    def finish(t):
        take(recv_sem.at[R_FIN, t], 2 * chunk)
        rows = rows_of(t, chip)
        total = (part[rows, :].astype(F32) + from_l[slot(t), :].astype(F32)) + from_r[slot(t), :].astype(F32)
        y_ref[rows, :] = (x_v[rows, :].astype(F32) + total).astype(BF16)
        for kind in (OUT_R, OUT_L, OUT_P):
            copy(kind, t).start()

    def spread(t):
        take(recv_sem.at[R_OUT, t], 2 * chunk)
        for kind in (FAR_R, FAR_L, P_LEFT, P_RIGHT):
            copy(kind, t).start()

    def far(t):
        take(recv_sem.at[R_FAR, t], chunk)
        for kind in (P_FAR_A, P_FAR_B):
            copy(kind, t).start()

    stages = {
        'chip_sum_a': lambda t: chip_sum(t, A, SWAP_A, FWD_R, OWN_L),
        'chip_sum_b': lambda t: chip_sum(t, B, SWAP_B, FWD_L, OWN_R),
        'pass_on_a': lambda t: pass_on(t, A, FWD_R, SUM_R, c_r),
        'pass_on_b': lambda t: pass_on(t, B, FWD_L, SUM_L, c_l),
        'finish': finish, 'spread': spread, 'far': far,
    }

    def place(p, s):
        for name, t in PLACES.get((s, p), ()):
            stages[name](t)

    def step(s):
        parts = {'project': lambda: project(s), 'scores': lambda: attend_scores(s), 'values': lambda: attend_values(s)}
        parts.update(('mlp%d' % j, functools.partial(mlp, s, j)) for j in range(ff_tiles))
        mlp_parts = ['mlp%d' % j for j in range(ff_tiles)]
        if s == 0:
            order = ['project', 'scores', 'values'] + mlp_parts
        else:
            order = ['project', mlp_parts[0], 'scores'] + mlp_parts[1:-1] + ['values', mlp_parts[-1]]
        place('start', s)
        for name in order:
            parts[name]()
            place(name, s)
        if s == 0:
            pl.semaphore_wait(barrier, 3)
        out_half(s, 0, SWAP_A)
        place('out0', s)
        out_half(s, 1, SWAP_B)
        place('out1', s)

    for s in range(blocks):
        step(s)
    for name, t in DRAIN:
        stages[name](t)
    take(done_sem.at[0], tokens // 2)
    take(send_sem.at[S_SWAP], tokens // 2)
    take(send_sem.at[S_LINK], tokens * 3 // 4)
    take(send_sem.at[S_PARTNER], tokens // 2)


def store_kernel(y_ref, k_ref, v_ref, y_hbm, k_hbm, v_hbm, sem):
    n = y_ref.shape[0] // STORES
    copies = [pltpu.make_async_copy(y_ref.at[pl.ds(i * n, n)], y_hbm.at[pl.ds(i * n, n)], sem.at[2 + i])
              for i in range(STORES)]
    copies += [pltpu.make_async_copy(k_ref, k_hbm, sem.at[0]), pltpu.make_async_copy(v_ref, v_hbm, sem.at[1])]
    for cp in copies:
        cp.start()
    for cp in copies:
        cp.wait()


def solution(mesh):
    n_tp = mesh.shape['tp']

    def local_layer(x_in, g_norm, w_q, w_k, w_v, w_o, w_gate, w_up, w_down):
        tokens, width = x_in.shape
        blocks = tokens // ROWS
        qw, ff = w_q.shape[1], w_gate.shape[1]
        heads = qw // HEAD_DIM
        half = ROWS // 2
        chunk = half // (n_tp // 2)
        cos_r, sin_r, cos_t, sin_t = rope_constants(ROWS, blocks)
        rope = np.stack([np.concatenate([cos_r, cos_t]), np.concatenate([sin_r, sin_t])])
        rope = jnp.asarray(np.pad(rope, ((0, 0), (0, -blocks % 8), (0, 0))))
        vm = lambda: pl.BlockSpec(memory_space=pltpu.VMEM)
        hbm = lambda: pl.BlockSpec(memory_space=pl.ANY)
        y_out, k_rot, v_proj = pl.pallas_call(
            functools.partial(layer_kernel, n_tp),
            out_shape=(pltpu.VMEM((tokens, width), BF16),
                       pltpu.VMEM((tokens, HEAD_DIM), BF16),
                       pltpu.VMEM((tokens, HEAD_DIM), BF16)),
            in_specs=[hbm()] * 10,
            out_specs=(vm(), vm(), vm()),
            scratch_shapes=[
                pltpu.VMEM((tokens, width), BF16),
                pltpu.VMEM((width,), BF16),
                pltpu.VMEM(rope.shape, F32),
                pltpu.VMEM((width, qw + 2 * HEAD_DIM), BF16),
                pltpu.VMEM((width, 2 * ff), BF16),
                pltpu.VMEM((qw + ff, width), BF16),
                pltpu.VMEM((ROWS, width), BF16),
                pltpu.VMEM((heads * ROWS, HEAD_DIM), BF16),
                pltpu.VMEM((tokens // ROWS, heads * ROWS, ROWS), F32),
                pltpu.VMEM((heads * ROWS, 128), F32),
                pltpu.VMEM((heads * ROWS, 128), F32),
                pltpu.VMEM((heads * ROWS, HEAD_DIM), F32),
                pltpu.VMEM((ROWS, qw + ff), BF16),
                pltpu.VMEM((tokens, width), BF16),
                pltpu.VMEM((tokens // 2, width), BF16),
                pltpu.VMEM((blocks * chunk, width), BF16),
                pltpu.VMEM((blocks * chunk, width), BF16),
                pltpu.VMEM((blocks * chunk, width), BF16),
                pltpu.SemaphoreType.DMA((5 + blocks,)),
                pltpu.SemaphoreType.DMA((3,)),
                pltpu.SemaphoreType.DMA((N_RECV, blocks)),
                pltpu.SemaphoreType.DMA((1,)),
            ],
            compiler_params=pltpu.CompilerParams(
                collective_id=0, has_side_effects=True, vmem_limit_bytes=52 * 2**20),
            name='layer',
        )(x_in, g_norm, w_q, w_k, w_v, w_o, w_gate, w_up, w_down, rope)
        y_out, k_rot, v_proj = pl.pallas_call(
            store_kernel,
            out_shape=tuple(jax.ShapeDtypeStruct(a.shape, BF16) for a in (y_out, k_rot, v_proj)),
            in_specs=[vm()] * 3, out_specs=(hbm(),) * 3,
            scratch_shapes=[pltpu.SemaphoreType.DMA((2 + STORES,))],
            compiler_params=pltpu.CompilerParams(vmem_limit_bytes=8 * 2**20),
            name='store',
        )(y_out, k_rot, v_proj)
        return y_out, k_rot.reshape(tokens, 1, HEAD_DIM), v_proj.reshape(tokens, 1, HEAD_DIM)

    return jax.shard_map(local_layer, mesh=mesh, in_specs=(P('dp', None), P(None), P(None, 'tp'), P(None, None), P(None, None), P('tp', None), P(None, 'tp'), P(None, 'tp'), P('tp', None)), out_specs=(P('dp', None), P('dp', 'tp', None), P('dp', 'tp', None)), check_vma=False)
```

```python
import functools
import math
import numpy as np
import jax
import jax.numpy as jnp
from jax import lax
from jax.experimental import pallas as pl
from jax.experimental.pallas import tpu as pltpu
from jax.sharding import PartitionSpec as P

HEAD_DIM = 128
ROPE_BASE = 500000.0
NORM_EPS = 1e-5
ROWS = 256
TILE = 256
STORES = 8
F32 = jnp.float32
BF16 = jnp.bfloat16
MESH = pl.DeviceIdType.MESH

(SWAP_A, SWAP_B, FWD_R, OWN_L, FWD_L, OWN_R, SUM_R, SUM_L, OUT_R, OUT_L, OUT_P, FAR_R, FAR_L,
 P_LEFT, P_RIGHT, P_FAR_A, P_FAR_B,
 END_R, END_L, END_RP, END_LP, P_END_A, P_END_B,
 FAR_R_HALF, FAR_L_HALF) = range(25)
R_SWAP_A, R_SWAP_B, R_FWD_R, R_FWD_L, R_FIN, R_OUT, R_FAR = range(7)
N_RECV = 7
ARRIVES = {SWAP_A: R_SWAP_A, SWAP_B: R_SWAP_B, FWD_R: R_FWD_R, FWD_L: R_FWD_L, OWN_L: R_FIN, OWN_R: R_FIN,
           SUM_R: R_FIN, SUM_L: R_FIN, OUT_R: R_OUT, OUT_L: R_OUT, FAR_R: R_FAR, FAR_L: R_FAR,
           FAR_R_HALF: R_FAR, FAR_L_HALF: R_FAR}
TO_PARTNER = (OUT_P, P_LEFT, P_RIGHT, P_FAR_A, P_FAR_B, P_END_A, P_END_B)
S_SWAP, S_LINK, S_PARTNER = range(3)
FWD_FIRST = (0,)

PLACES = {
    (1, 'project'): (('chip_sum_a', 0), ('chip_sum_b', 0),),
    (1, 'out1'): (('pass_on_a', 0), ('pass_on_b', 0), ('chip_sum_a', 1),),
    (2, 'project'): (('chip_sum_b', 1),),
    (2, 'mlp2'): (('finish', 0),),
    (2, 'out1'): (('pass_on_a', 1), ('pass_on_b', 1), ('chip_sum_b', 2),),
    (3, 'project'): (('chip_sum_a', 2),),
    (3, 'mlp2'): (('spread', 0), ('finish', 1), ('pass_on_b', 2),),
    (3, 'out1'): (('pass_on_a', 2),),
    (4, 'project'): (('chip_sum_a', 3), ('chip_sum_b', 3),),
    (4, 'out1'): (('finish', 2), ('chip_sum_a', 4),),
    (5, 'project'): (('spread', 1),),
    (5, 'mlp2'): (('spread', 2), ('chip_sum_b', 4),),
    (5, 'out1'): (('chip_sum_a', 5), ('chip_sum_b', 5),),
}
DRAIN = (
    ('pass_on_a', 3), ('pass_on_a', 4), ('pass_on_b', 3), ('far', 0),
    ('far', 1), ('far', 2), ('pass_on_b', 4), ('pass_on_a', 5),
    ('pass_on_b', 5), ('finish', 3), ('finish', 4), ('finish', 5),
    ('spread', 3), ('spread', 4), ('spread', 5), ('far', 3),
    ('far', 4), ('far', 5),
)


def rope_constants(rows, blocks):
    inv_freq = ROPE_BASE ** (-np.arange(0, HEAD_DIM, 2, dtype=np.float64) / HEAD_DIM)
    def tables(positions):
        ang = positions[:, None] * inv_freq[None, :]
        cos, sin = np.cos(ang), np.sin(ang)
        return (np.concatenate([cos, cos], 1).astype(np.float32),
                np.concatenate([-sin, sin], 1).astype(np.float32))
    cos_r, sin_r = tables(np.arange(rows, dtype=np.float64))
    cos_t, sin_t = tables(np.arange(blocks, dtype=np.float64) * rows)
    return cos_r, sin_r, cos_t, sin_t


def layer_kernel(n_tp, x_hbm, g_hbm, wq_hbm, wk_hbm, wv_hbm, wo_hbm, wg_hbm, wu_hbm, wd_hbm,
                 rope_hbm, y_ref, k_ref, v_ref,
                 x_v, g_v, rope, wqkv, wgu, wod, a_s, q_s, s_s, m_s, l_s, o_s, om_s,
                 part, swap, fwd, from_l, from_r, load_sem, send_sem, recv_sem, done_sem):
    tokens, width = x_v.shape
    blocks = tokens // ROWS
    half = ROWS // 2
    n_chip = n_tp // 2
    chunk = half // n_chip
    wh = width // 2
    qw = wq_hbm.shape[1]
    heads = qw // HEAD_DIM
    ff = wg_hbm.shape[1]
    me = lax.axis_index('tp')
    chip, core = me // 2, lax.rem(me, 2)
    partner = chip * 2 + 1 - core
    c_r = lax.rem(chip + 1, n_chip)
    c_l = lax.rem(chip + n_chip - 1, n_chip)
    c_o = lax.rem(chip + 2, n_chip)
    right = c_r * 2 + core
    left = c_l * 2 + core
    right_p, left_p = c_r * 2 + 1 - core, c_l * 2 + 1 - core

    A, B = pl.ds(0, wh), pl.ds(wh, wh)
    A1, A2, B1, B2 = (pl.ds(i * wh // 2, wh // 2) for i in range(4))

    kv_col = pl.multiple_of(me * HEAD_DIM, HEAD_DIM)
    def x_load(t):
        rows = pl.ds(pl.multiple_of(t * ROWS, ROWS), ROWS)
        return pltpu.make_async_copy(x_hbm.at[rows], x_v.at[rows], load_sem.at[4 + ff // TILE + t])
    def load(i, src, dst):
        return pltpu.make_async_copy(src, dst, load_sem.at[i])
    ff_tiles = ff // TILE
    L_SMALL, L_QKV, L_OUT, L_MLP, L_X = 0, 2, 3, 4, 4 + ff_tiles
    small_loads = [load(L_SMALL, g_hbm, g_v), load(L_SMALL + 1, rope_hbm, rope)]
    qkv_loads = [
        load(L_QKV, wq_hbm, wqkv.at[:, pl.ds(0, qw)]),
        load(L_QKV, wk_hbm.at[:, pl.ds(kv_col, HEAD_DIM)], wqkv.at[:, pl.ds(qw, HEAD_DIM)]),
        load(L_QKV, wv_hbm.at[:, pl.ds(kv_col, HEAD_DIM)], wqkv.at[:, pl.ds(qw + HEAD_DIM, HEAD_DIM)]),
    ]
    mlp_loads = []
    for j in range(ff_tiles):
        cols, up_cols = pl.ds(j * TILE, TILE), pl.ds(ff + j * TILE, TILE)
        mlp_loads += [load(L_MLP + j, wg_hbm.at[:, cols], wgu.at[:, cols]),
                      load(L_MLP + j, wu_hbm.at[:, cols], wgu.at[:, up_cols])]
    out_loads = [load(L_OUT, wo_hbm, wod.at[pl.ds(0, qw)]), load(L_OUT, wd_hbm, wod.at[pl.ds(qw, ff)])]
    x_load(0).start()
    for cp in small_loads + qkv_loads + mlp_loads + out_loads:
        cp.start()
    for t in range(1, blocks):
        x_load(t).start()

    def loaded(t, sem, ref):
        if t == 0:
            load(sem, ref, ref).wait()

    barrier = pltpu.get_barrier_semaphore()
    for dev in (partner, left, right, left_p, right_p):
        pl.semaphore_signal(barrier, inc=1, device_id={'tp': dev}, device_id_type=MESH)
    def rows_of(t, c):
        return pl.ds(pl.multiple_of(t * ROWS + core * half + c * chunk, chunk), chunk)

    def slot(t):
        return pl.ds(pl.multiple_of(t * chunk, chunk), chunk)

    def copy(kind, t):
        other = pl.ds(pl.multiple_of(t * ROWS + (1 - core) * half, half), half)
        def y_copy(c, cols, dev):
            return y_ref.at[rows_of(t, c), cols], y_ref.at[rows_of(t, c), cols], dev
        src, dst, dev = {
            SWAP_A: lambda: (part.at[other, A], swap.at[pl.ds(pl.multiple_of(t * half, half), half), A], partner),
            SWAP_B: lambda: (part.at[other, B], swap.at[pl.ds(pl.multiple_of(t * half, half), half), B], partner),
            FWD_R: lambda: (part.at[rows_of(t, c_o), A], fwd.at[slot(t), A], right),
            OWN_R: lambda: (part.at[rows_of(t, c_r), B], from_l.at[slot(t), B], right),
            FWD_L: lambda: (part.at[rows_of(t, c_o), B], fwd.at[slot(t), B], left),
            OWN_L: lambda: (part.at[rows_of(t, c_l), A], from_r.at[slot(t), A], left),
            SUM_R: lambda: (part.at[rows_of(t, c_r), A], from_l.at[slot(t), A], right),
            SUM_L: lambda: (part.at[rows_of(t, c_l), B], from_r.at[slot(t), B], left),
            OUT_R: lambda: (y_ref.at[rows_of(t, chip)], y_ref.at[rows_of(t, chip)], right),
            OUT_L: lambda: (y_ref.at[rows_of(t, chip)], y_ref.at[rows_of(t, chip)], left),
            OUT_P: lambda: (y_ref.at[rows_of(t, chip)], y_ref.at[rows_of(t, chip)], partner),
            FAR_R: lambda: (y_ref.at[rows_of(t, c_l), A], y_ref.at[rows_of(t, c_l), A], right),
            FAR_L: lambda: (y_ref.at[rows_of(t, c_r), B], y_ref.at[rows_of(t, c_r), B], left),
            P_LEFT: lambda: (y_ref.at[rows_of(t, c_l)], y_ref.at[rows_of(t, c_l)], partner),
            P_RIGHT: lambda: (y_ref.at[rows_of(t, c_r)], y_ref.at[rows_of(t, c_r)], partner),
            P_FAR_A: lambda: (y_ref.at[rows_of(t, c_o), A], y_ref.at[rows_of(t, c_o), A], partner),
            P_FAR_B: lambda: (y_ref.at[rows_of(t, c_o), B], y_ref.at[rows_of(t, c_o), B], partner),
            FAR_R_HALF: lambda: y_copy(c_l, A1, right),
            FAR_L_HALF: lambda: y_copy(c_r, B1, left),
            END_R: lambda: y_copy(c_l, A2, right),
            END_L: lambda: y_copy(c_r, B2, left),
            END_RP: lambda: y_copy(c_l, A2, right_p),
            END_LP: lambda: y_copy(c_r, B2, left_p),
            P_END_A: lambda: y_copy(c_o, A1, partner),
            P_END_B: lambda: y_copy(c_o, B1, partner),
        }[kind]()
        leaves = S_SWAP if kind in (SWAP_A, SWAP_B) else S_PARTNER if kind in TO_PARTNER else S_LINK
        return pltpu.make_async_remote_copy(
            src_ref=src, dst_ref=dst, send_sem=send_sem.at[leaves],
            recv_sem=recv_sem.at[ARRIVES[kind], t] if kind in ARRIVES else done_sem.at[0],
            device_id={'tp': dev}, device_id_type=MESH)

    def take(sem, rows):
        ref = y_ref.at[pl.ds(0, rows)]
        pltpu.make_async_copy(ref, ref, sem).wait()

    scale = 1.0 / math.sqrt(HEAD_DIM) * math.log2(math.e)

    def project(t):
        if t == 0:
            for cp in small_loads:
                cp.wait()
        x_load(t).wait()
        step = 64
        gain = g_v[...].astype(F32).reshape(1, width)
        for i in range(ROWS // step):
            xf = x_v[pl.ds(pl.multiple_of(t * ROWS + i * step, step), step), :].astype(F32)
            inv = lax.rsqrt(jnp.mean(xf * xf, axis=-1, keepdims=True) + NORM_EPS)
            a_s[pl.ds(i * step, step), :] = (xf * inv * gain).astype(BF16)
        loaded(t, L_QKV, wqkv)
        a = a_s[...]
        c0, s0 = rope[0, pl.ds(ROWS + t, 1), :], rope[1, pl.ds(ROWS + t, 1), :]
        cos_r, sin_r = rope[0, :ROWS, :], rope[1, :ROWS, :]
        cos = cos_r * c0 - sin_r * s0
        sin = sin_r * c0 + cos_r * s0
        rot = lambda p: (p * cos + pltpu.roll(p, HEAD_DIM // 2, 1) * sin).astype(BF16)
        q = jnp.dot(a, wqkv[:, pl.ds(0, qw)], preferred_element_type=F32)
        kv = jnp.dot(a, wqkv[:, pl.ds(qw, 2 * HEAD_DIM)], preferred_element_type=F32)
        for h in range(heads):
            q_s[pl.ds(h * ROWS, ROWS), :] = rot(q[:, h * HEAD_DIM:(h + 1) * HEAD_DIM])
        rows = pl.ds(pl.multiple_of(t * ROWS, ROWS), ROWS)
        k_ref[rows, :] = rot(kv[:, :HEAD_DIM])
        v_ref[rows, :] = kv[:, HEAD_DIM:].astype(BF16)

    def lanes(op, s):
        acc = s[:, :128]
        for i in range(1, ROWS // 128):
            acc = op(acc, s[:, i * 128:(i + 1) * 128])
        return acc

    def keys(kb):
        return pl.ds(pl.multiple_of(kb * ROWS, ROWS), ROWS)

    def score(kb):
        return lax.dot_general(q_s[...], k_ref[keys(kb), :], (((1,), (1,)), ((), ())), preferred_element_type=F32)

    def attend_scores(t):
        s = score(t)
        shape = (heads, ROWS, ROWS)
        q_pos = lax.broadcasted_iota(jnp.int32, shape, 1).reshape(heads * ROWS, ROWS)
        k_pos = lax.broadcasted_iota(jnp.int32, shape, 2).reshape(heads * ROWS, ROWS)
        s = jnp.where(k_pos <= q_pos, s, -1e30)
        s_s[t] = s
        m_s[...] = lanes(jnp.maximum, s)

        for kb in range(t):
            s = score(kb)
            s_s[kb] = s
            m_s[...] = jnp.maximum(m_s[...], lanes(jnp.maximum, s))
        m_s[...] = jnp.broadcast_to(jnp.max(m_s[...], axis=-1, keepdims=True) * scale, m_s.shape)
        l_s[...] = jnp.zeros_like(l_s)

        for kb in range(t + 1):
            m = m_s[...]
            p = jnp.exp2(s_s[kb] * scale - jnp.concatenate([m] * (ROWS // 128), axis=1))
            s_s[kb] = p
            l_s[...] += lanes(jnp.add, p)

    def attend_values(t):
        l_s[...] = jnp.broadcast_to(1.0 / jnp.sum(l_s[...], axis=-1, keepdims=True), l_s.shape)
        o_s[...] = jnp.zeros_like(o_s)

        for kb in range(t + 1):
            r = l_s[...]
            p = (s_s[kb] * jnp.concatenate([r] * (ROWS // 128), axis=1)).astype(BF16)
            o_s[...] += jnp.dot(p, v_ref[keys(kb), :], preferred_element_type=F32)
        for h in range(heads):
            om_s[:, pl.ds(h * HEAD_DIM, HEAD_DIM)] = o_s[pl.ds(h * ROWS, ROWS), :].astype(BF16)

    def mlp(t, j):
        loaded(t, L_MLP + j, wgu.at[:, pl.ds(0, 2 * TILE)])
        a = a_s[...]
        gate = jnp.dot(a, wgu[:, pl.ds(j * TILE, TILE)], preferred_element_type=F32)
        up = jnp.dot(a, wgu[:, pl.ds(ff + j * TILE, TILE)], preferred_element_type=F32)
        om_s[:, pl.ds(qw + j * TILE, TILE)] = (jax.nn.silu(gate) * up).astype(BF16)

    def out_half(t, which, kind):
        if which == 0:
            loaded(t, L_OUT, wod)
        om = om_s[...]
        rows = pl.ds(pl.multiple_of(t * ROWS, ROWS), ROWS)
        tiles = width // TILE // 2
        for j in range(which * tiles, (which + 1) * tiles):
            cols = pl.ds(j * TILE, TILE)
            part[rows, cols] = jnp.dot(om, wod[:, cols], preferred_element_type=F32).astype(BF16)
        copy(kind, t).start()

    def chip_sum(t, cols, got, *sends):
        copy(got, t).wait_recv()
        for i in range(4):
            n = half // 4
            rows = pl.ds(pl.multiple_of(t * ROWS + core * half + i * n, n), n)
            other = swap[pl.ds(pl.multiple_of(t * half + i * n, n), n), cols].astype(F32)
            part[rows, cols] = (part[rows, cols].astype(F32) + other).astype(BF16)
        for kind in sends:
            copy(kind, t).start()

    def pass_on(t, cols, got, out, c):
        copy(got, t).wait_recv()
        rows = rows_of(t, c)
        part[rows, cols] = (part[rows, cols].astype(F32) + fwd[slot(t), cols].astype(F32)).astype(BF16)
        copy(out, t).start()

    def finish(t):
        take(recv_sem.at[R_FIN, t], 2 * chunk)
        rows = rows_of(t, chip)
        total = (part[rows, :].astype(F32) + from_l[slot(t), :].astype(F32)) + from_r[slot(t), :].astype(F32)
        y_ref[rows, :] = (x_v[rows, :].astype(F32) + total).astype(BF16)
        for kind in (OUT_R, OUT_L, OUT_P):
            copy(kind, t).start()

    last = blocks - 1

    def spread(t):
        take(recv_sem.at[R_OUT, t], 2 * chunk)
        far_kinds = (FAR_R, FAR_L) if t < last else (FAR_R_HALF, FAR_L_HALF, END_RP, END_LP, END_R, END_L)
        for kind in far_kinds + (P_LEFT, P_RIGHT):
            copy(kind, t).start()

    def far(t):
        take(recv_sem.at[R_FAR, t], chunk if t < last else chunk // 2)
        for kind in (P_FAR_A, P_FAR_B) if t < last else (P_END_A, P_END_B):
            copy(kind, t).start()

    stages = {
        'chip_sum_a': lambda t: chip_sum(t, A, SWAP_A, *((FWD_R,) if t in FWD_FIRST else (FWD_R, OWN_L))),
        'chip_sum_b': lambda t: chip_sum(t, B, SWAP_B, *((FWD_L, OWN_R, OWN_L) if t in FWD_FIRST else (FWD_L, OWN_R))),
        'pass_on_a': lambda t: pass_on(t, A, FWD_R, SUM_R, c_r),
        'pass_on_b': lambda t: pass_on(t, B, FWD_L, SUM_L, c_l),
        'finish': finish, 'spread': spread, 'far': far,
    }

    def place(p, s):
        for name, t in PLACES.get((s, p), ()):
            stages[name](t)

    def step(s):
        parts = {'project': lambda: project(s), 'scores': lambda: attend_scores(s), 'values': lambda: attend_values(s)}
        parts.update(('mlp%d' % j, functools.partial(mlp, s, j)) for j in range(ff_tiles))
        mlp_parts = ['mlp%d' % j for j in range(ff_tiles)]
        order = ['project', mlp_parts[0], 'scores'] + mlp_parts[1:-1] + ['values', mlp_parts[-1]]
        place('start', s)
        for name in order:
            parts[name]()
            place(name, s)
        if s == 0:
            pl.semaphore_wait(barrier, 5)
        out_half(s, 0, SWAP_A)
        place('out0', s)
        out_half(s, 1, SWAP_B)
        place('out1', s)

    for s in range(blocks):
        step(s)
    for name, t in DRAIN:
        stages[name](t)
    take(done_sem.at[0], tokens // 2 + chunk // 2)
    take(send_sem.at[S_SWAP], tokens // 2)
    take(send_sem.at[S_LINK], tokens * 3 // 4 + chunk // 2)
    take(send_sem.at[S_PARTNER], tokens // 2 - chunk // 2)


def store_kernel(y_ref, k_ref, v_ref, y_hbm, k_hbm, v_hbm, sem):
    n = y_ref.shape[0] // STORES
    copies = [pltpu.make_async_copy(y_ref.at[pl.ds(i * n, n)], y_hbm.at[pl.ds(i * n, n)], sem.at[2 + i])
              for i in range(STORES)]
    copies += [pltpu.make_async_copy(k_ref, k_hbm, sem.at[0]), pltpu.make_async_copy(v_ref, v_hbm, sem.at[1])]
    for cp in copies:
        cp.start()
    for cp in copies:
        cp.wait()


def solution(mesh):
    n_tp = mesh.shape['tp']

    def local_layer(x_in, g_norm, w_q, w_k, w_v, w_o, w_gate, w_up, w_down):
        tokens, width = x_in.shape
        blocks = tokens // ROWS
        qw, ff = w_q.shape[1], w_gate.shape[1]
        heads = qw // HEAD_DIM
        half = ROWS // 2
        chunk = half // (n_tp // 2)
        cos_r, sin_r, cos_t, sin_t = rope_constants(ROWS, blocks)
        rope = np.stack([np.concatenate([cos_r, cos_t]), np.concatenate([sin_r, sin_t])])
        rope = jnp.asarray(np.pad(rope, ((0, 0), (0, -blocks % 8), (0, 0))))
        vm = lambda: pl.BlockSpec(memory_space=pltpu.VMEM)
        hbm = lambda: pl.BlockSpec(memory_space=pl.ANY)
        y_out, k_rot, v_proj = pl.pallas_call(
            functools.partial(layer_kernel, n_tp),
            out_shape=(pltpu.VMEM((tokens, width), BF16),
                       pltpu.VMEM((tokens, HEAD_DIM), BF16),
                       pltpu.VMEM((tokens, HEAD_DIM), BF16)),
            in_specs=[hbm()] * 10,
            out_specs=(vm(), vm(), vm()),
            scratch_shapes=[
                pltpu.VMEM((tokens, width), BF16),
                pltpu.VMEM((width,), BF16),
                pltpu.VMEM(rope.shape, F32),
                pltpu.VMEM((width, qw + 2 * HEAD_DIM), BF16),
                pltpu.VMEM((width, 2 * ff), BF16),
                pltpu.VMEM((qw + ff, width), BF16),
                pltpu.VMEM((ROWS, width), BF16),
                pltpu.VMEM((heads * ROWS, HEAD_DIM), BF16),
                pltpu.VMEM((tokens // ROWS, heads * ROWS, ROWS), F32),
                pltpu.VMEM((heads * ROWS, 128), F32),
                pltpu.VMEM((heads * ROWS, 128), F32),
                pltpu.VMEM((heads * ROWS, HEAD_DIM), F32),
                pltpu.VMEM((ROWS, qw + ff), BF16),
                pltpu.VMEM((tokens, width), BF16),
                pltpu.VMEM((tokens // 2, width), BF16),
                pltpu.VMEM((blocks * chunk, width), BF16),
                pltpu.VMEM((blocks * chunk, width), BF16),
                pltpu.VMEM((blocks * chunk, width), BF16),
                pltpu.SemaphoreType.DMA((4 + ff // TILE + blocks,)),
                pltpu.SemaphoreType.DMA((3,)),
                pltpu.SemaphoreType.DMA((N_RECV, blocks)),
                pltpu.SemaphoreType.DMA((1,)),
            ],
            compiler_params=pltpu.CompilerParams(
                collective_id=0, has_side_effects=True, vmem_limit_bytes=52 * 2**20),
            name='layer',
        )(x_in, g_norm, w_q, w_k, w_v, w_o, w_gate, w_up, w_down, rope)
        y_out, k_rot, v_proj = pl.pallas_call(
            store_kernel,
            out_shape=tuple(jax.ShapeDtypeStruct(a.shape, BF16) for a in (y_out, k_rot, v_proj)),
            in_specs=[vm()] * 3, out_specs=(hbm(),) * 3,
            scratch_shapes=[pltpu.SemaphoreType.DMA((2 + STORES,))],
            compiler_params=pltpu.CompilerParams(vmem_limit_bytes=8 * 2**20),
            name='store',
        )(y_out, k_rot, v_proj)
        return y_out, k_rot.reshape(tokens, 1, HEAD_DIM), v_proj.reshape(tokens, 1, HEAD_DIM)

    return jax.shard_map(local_layer, mesh=mesh, in_specs=(P('dp', None), P(None), P(None, 'tp'), P(None, None), P(None, None), P('tp', None), P(None, 'tp'), P(None, 'tp'), P('tp', None)), out_specs=(P('dp', None), P('dp', 'tp', None), P('dp', 'tp', None)), check_vma=False)
```

```python
import functools
import math
import numpy as np
import jax
import jax.numpy as jnp
from jax import lax
from jax.experimental import pallas as pl
from jax.experimental.pallas import tpu as pltpu
from jax.sharding import PartitionSpec as P

HEAD_DIM = 128
ROPE_BASE = 500000.0
NORM_EPS = 1e-5
ROWS = 256
TILE = 256
STORES = 1
F32 = jnp.float32
BF16 = jnp.bfloat16
MESH = pl.DeviceIdType.MESH

(SWAP_A, SWAP_B, FWD_R, OWN_L, FWD_L, OWN_R, SUM_R, SUM_L, OUT_R, OUT_L, OUT_P, FAR_R, FAR_L,
 P_LEFT, P_RIGHT, P_FAR_A, P_FAR_B,
 END_R, END_L, END_RP, END_LP, P_END_A, P_END_B,
 FAR_R_HALF, FAR_L_HALF) = range(25)
R_SWAP_A, R_SWAP_B, R_FWD_R, R_FWD_L, R_FIN, R_OUT, R_FAR = range(7)
N_RECV = 7
ARRIVES = {SWAP_A: R_SWAP_A, SWAP_B: R_SWAP_B, FWD_R: R_FWD_R, FWD_L: R_FWD_L, OWN_L: R_FIN, OWN_R: R_FIN,
           SUM_R: R_FIN, SUM_L: R_FIN, OUT_R: R_OUT, OUT_L: R_OUT, FAR_R: R_FAR, FAR_L: R_FAR,
           FAR_R_HALF: R_FAR, FAR_L_HALF: R_FAR}
TO_PARTNER = (OUT_P, P_LEFT, P_RIGHT, P_FAR_A, P_FAR_B, P_END_A, P_END_B)
S_SWAP, S_LINK, S_PARTNER = range(3)
FWD_FIRST = (0,)

PLACES = {
    (1, 'project'): (('chip_sum_a', 0), ('chip_sum_b', 0),),
    (1, 'out1'): (('pass_on_a', 0), ('pass_on_b', 0), ('chip_sum_a', 1),),
    (2, 'project'): (('chip_sum_b', 1),),
    (2, 'mlp2'): (('finish', 0),),
    (2, 'out1'): (('pass_on_a', 1), ('pass_on_b', 1), ('chip_sum_b', 2),),
    (3, 'project'): (('chip_sum_a', 2),),
    (3, 'mlp2'): (('spread', 0), ('finish', 1),),
    (3, 'out1'): (('pass_on_b', 2), ('pass_on_a', 2),),
    (4, 'project'): (('chip_sum_a', 3), ('chip_sum_b', 3),),
    (4, 'out1'): (('finish', 2), ('chip_sum_a', 4),),
    (5, 'project'): (('spread', 1),),
    (5, 'mlp2'): (('spread', 2), ('chip_sum_b', 4),),
    (5, 'out1'): (('chip_sum_a', 5), ('chip_sum_b', 5),),
}
DRAIN = (
    ('pass_on_a', 3), ('pass_on_a', 4), ('pass_on_b', 3), ('far', 0),
    ('far', 1), ('far', 2), ('pass_on_b', 4), ('pass_on_a', 5),
    ('pass_on_b', 5), ('finish', 3), ('finish', 4), ('finish', 5),
    ('spread', 3), ('spread', 4), ('spread', 5), ('far', 3),
    ('far', 4), ('far', 5),
)


def rope_constants(rows, blocks):
    inv_freq = ROPE_BASE ** (-np.arange(0, HEAD_DIM, 2, dtype=np.float64) / HEAD_DIM)
    def tables(positions):
        ang = positions[:, None] * inv_freq[None, :]
        cos, sin = np.cos(ang), np.sin(ang)
        return (np.concatenate([cos, cos], 1).astype(np.float32),
                np.concatenate([-sin, sin], 1).astype(np.float32))
    cos_r, sin_r = tables(np.arange(rows, dtype=np.float64))
    cos_t, sin_t = tables(np.arange(blocks, dtype=np.float64) * rows)
    return cos_r, sin_r, cos_t, sin_t


def layer_kernel(n_tp, x_hbm, g_hbm, wq_hbm, wk_hbm, wv_hbm, wo_hbm, wg_hbm, wu_hbm, wd_hbm,
                 rope_hbm, y_ref, k_ref, v_ref,
                 x_v, g_v, rope, wqkv, wgu, wod, a_s, q_s, s_s, m_s, l_s, o_s, om_s,
                 part, swap, fwd, from_l, from_r, load_sem, send_sem, recv_sem, done_sem):
    tokens, width = x_v.shape
    blocks = tokens // ROWS
    half = ROWS // 2
    n_chip = n_tp // 2
    chunk = half // n_chip
    wh = width // 2
    qw = wq_hbm.shape[1]
    heads = qw // HEAD_DIM
    ff = wg_hbm.shape[1]
    me = lax.axis_index('tp')
    chip, core = me // 2, lax.rem(me, 2)
    partner = chip * 2 + 1 - core
    c_r = lax.rem(chip + 1, n_chip)
    c_l = lax.rem(chip + n_chip - 1, n_chip)
    c_o = lax.rem(chip + 2, n_chip)
    right = c_r * 2 + core
    left = c_l * 2 + core
    right_p, left_p = c_r * 2 + 1 - core, c_l * 2 + 1 - core

    A, B = pl.ds(0, wh), pl.ds(wh, wh)
    A1, A2, B1, B2 = (pl.ds(i * wh // 2, wh // 2) for i in range(4))

    kv_col = pl.multiple_of(me * HEAD_DIM, HEAD_DIM)
    def x_load(t):
        rows = pl.ds(pl.multiple_of(t * ROWS, ROWS), ROWS)
        return pltpu.make_async_copy(x_hbm.at[rows], x_v.at[rows], load_sem.at[4 + ff // TILE + t])
    def load(i, src, dst):
        return pltpu.make_async_copy(src, dst, load_sem.at[i])
    ff_tiles = ff // TILE
    L_SMALL, L_QKV, L_OUT, L_MLP, L_X = 0, 2, 3, 4, 4 + ff_tiles
    small_loads = [load(L_SMALL, g_hbm, g_v), load(L_SMALL + 1, rope_hbm, rope)]
    qkv_loads = [
        load(L_QKV, wq_hbm, wqkv.at[:, pl.ds(0, qw)]),
        load(L_QKV, wk_hbm.at[:, pl.ds(kv_col, HEAD_DIM)], wqkv.at[:, pl.ds(qw, HEAD_DIM)]),
        load(L_QKV, wv_hbm.at[:, pl.ds(kv_col, HEAD_DIM)], wqkv.at[:, pl.ds(qw + HEAD_DIM, HEAD_DIM)]),
    ]
    mlp_loads = []
    for j in range(ff_tiles):
        cols, up_cols = pl.ds(j * TILE, TILE), pl.ds(ff + j * TILE, TILE)
        mlp_loads += [load(L_MLP + j, wg_hbm.at[:, cols], wgu.at[:, cols]),
                      load(L_MLP + j, wu_hbm.at[:, cols], wgu.at[:, up_cols])]
    out_loads = [load(L_OUT, wo_hbm, wod.at[pl.ds(0, qw)]), load(L_OUT, wd_hbm, wod.at[pl.ds(qw, ff)])]
    x_load(0).start()
    for cp in small_loads + qkv_loads + mlp_loads + out_loads:
        cp.start()
    for t in range(1, blocks):
        x_load(t).start()

    def loaded(t, sem, ref):
        if t == 0:
            load(sem, ref, ref).wait()

    barrier = pltpu.get_barrier_semaphore()
    for dev in (partner, left, right, left_p, right_p):
        pl.semaphore_signal(barrier, inc=1, device_id={'tp': dev}, device_id_type=MESH)
    def rows_of(t, c):
        return pl.ds(pl.multiple_of(t * ROWS + core * half + c * chunk, chunk), chunk)

    def slot(t):
        return pl.ds(pl.multiple_of(t * chunk, chunk), chunk)

    def copy(kind, t):
        other = pl.ds(pl.multiple_of(t * ROWS + (1 - core) * half, half), half)
        def y_copy(c, cols, dev):
            return y_ref.at[rows_of(t, c), cols], y_ref.at[rows_of(t, c), cols], dev
        src, dst, dev = {
            SWAP_A: lambda: (part.at[other, A], swap.at[pl.ds(pl.multiple_of(t * half, half), half), A], partner),
            SWAP_B: lambda: (part.at[other, B], swap.at[pl.ds(pl.multiple_of(t * half, half), half), B], partner),
            FWD_R: lambda: (part.at[rows_of(t, c_o), A], fwd.at[slot(t), A], right),
            OWN_R: lambda: (part.at[rows_of(t, c_r), B], from_l.at[slot(t), B], right),
            FWD_L: lambda: (part.at[rows_of(t, c_o), B], fwd.at[slot(t), B], left),
            OWN_L: lambda: (part.at[rows_of(t, c_l), A], from_r.at[slot(t), A], left),
            SUM_R: lambda: (part.at[rows_of(t, c_r), A], from_l.at[slot(t), A], right),
            SUM_L: lambda: (part.at[rows_of(t, c_l), B], from_r.at[slot(t), B], left),
            OUT_R: lambda: (y_ref.at[rows_of(t, chip)], y_ref.at[rows_of(t, chip)], right),
            OUT_L: lambda: (y_ref.at[rows_of(t, chip)], y_ref.at[rows_of(t, chip)], left),
            OUT_P: lambda: (y_ref.at[rows_of(t, chip)], y_ref.at[rows_of(t, chip)], partner),
            FAR_R: lambda: (y_ref.at[rows_of(t, c_l), A], y_ref.at[rows_of(t, c_l), A], right),
            FAR_L: lambda: (y_ref.at[rows_of(t, c_r), B], y_ref.at[rows_of(t, c_r), B], left),
            P_LEFT: lambda: (y_ref.at[rows_of(t, c_l)], y_ref.at[rows_of(t, c_l)], partner),
            P_RIGHT: lambda: (y_ref.at[rows_of(t, c_r)], y_ref.at[rows_of(t, c_r)], partner),
            P_FAR_A: lambda: (y_ref.at[rows_of(t, c_o), A], y_ref.at[rows_of(t, c_o), A], partner),
            P_FAR_B: lambda: (y_ref.at[rows_of(t, c_o), B], y_ref.at[rows_of(t, c_o), B], partner),
            FAR_R_HALF: lambda: y_copy(c_l, A1, right),
            FAR_L_HALF: lambda: y_copy(c_r, B1, left),
            END_R: lambda: y_copy(c_l, A2, right),
            END_L: lambda: y_copy(c_r, B2, left),
            END_RP: lambda: y_copy(c_l, A2, right_p),
            END_LP: lambda: y_copy(c_r, B2, left_p),
            P_END_A: lambda: y_copy(c_o, A1, partner),
            P_END_B: lambda: y_copy(c_o, B1, partner),
        }[kind]()
        leaves = S_SWAP if kind in (SWAP_A, SWAP_B) else S_PARTNER if kind in TO_PARTNER else S_LINK
        return pltpu.make_async_remote_copy(
            src_ref=src, dst_ref=dst, send_sem=send_sem.at[leaves],
            recv_sem=recv_sem.at[ARRIVES[kind], t] if kind in ARRIVES else done_sem.at[0],
            device_id={'tp': dev}, device_id_type=MESH)

    def take(sem, rows):
        ref = y_ref.at[pl.ds(0, rows)]
        pltpu.make_async_copy(ref, ref, sem).wait()

    scale = 1.0 / math.sqrt(HEAD_DIM) * math.log2(math.e)

    def project(t):
        if t == 0:
            for cp in small_loads:
                cp.wait()
        x_load(t).wait()
        step = 64
        gain = g_v[...].astype(F32).reshape(1, width)
        for i in range(ROWS // step):
            xf = x_v[pl.ds(pl.multiple_of(t * ROWS + i * step, step), step), :].astype(F32)
            inv = lax.rsqrt(jnp.mean(xf * xf, axis=-1, keepdims=True) + NORM_EPS)
            a_s[pl.ds(i * step, step), :] = (xf * inv * gain).astype(BF16)
        loaded(t, L_QKV, wqkv)
        a = a_s[...]
        c0, s0 = rope[0, pl.ds(ROWS + t, 1), :], rope[1, pl.ds(ROWS + t, 1), :]
        cos_r, sin_r = rope[0, :ROWS, :], rope[1, :ROWS, :]
        cos = cos_r * c0 - sin_r * s0
        sin = sin_r * c0 + cos_r * s0
        rot = lambda p: (p * cos + pltpu.roll(p, HEAD_DIM // 2, 1) * sin).astype(BF16)
        q = jnp.dot(a, wqkv[:, pl.ds(0, qw)], preferred_element_type=F32)
        kv = jnp.dot(a, wqkv[:, pl.ds(qw, 2 * HEAD_DIM)], preferred_element_type=F32)
        for h in range(heads):
            q_s[pl.ds(h * ROWS, ROWS), :] = rot(q[:, h * HEAD_DIM:(h + 1) * HEAD_DIM])
        rows = pl.ds(pl.multiple_of(t * ROWS, ROWS), ROWS)
        k_ref[rows, :] = rot(kv[:, :HEAD_DIM])
        v_ref[rows, :] = kv[:, HEAD_DIM:].astype(BF16)

    def lanes(op, s):
        acc = s[:, :128]
        for i in range(1, ROWS // 128):
            acc = op(acc, s[:, i * 128:(i + 1) * 128])
        return acc

    def keys(kb):
        return pl.ds(pl.multiple_of(kb * ROWS, ROWS), ROWS)

    def score(kb):
        return lax.dot_general(q_s[...], k_ref[keys(kb), :], (((1,), (1,)), ((), ())), preferred_element_type=F32)

    def attend_scores(t):
        s = score(t)
        shape = (heads, ROWS, ROWS)
        q_pos = lax.broadcasted_iota(jnp.int32, shape, 1).reshape(heads * ROWS, ROWS)
        k_pos = lax.broadcasted_iota(jnp.int32, shape, 2).reshape(heads * ROWS, ROWS)
        s = jnp.where(k_pos <= q_pos, s, -1e30)
        s_s[t] = s
        m_s[...] = lanes(jnp.maximum, s)

        for kb in range(t):
            s = score(kb)
            s_s[kb] = s
            m_s[...] = jnp.maximum(m_s[...], lanes(jnp.maximum, s))
        m_s[...] = jnp.broadcast_to(jnp.max(m_s[...], axis=-1, keepdims=True) * scale, m_s.shape)
        l_s[...] = jnp.zeros_like(l_s)

        for kb in range(t + 1):
            m = m_s[...]
            p = jnp.exp2(s_s[kb] * scale - jnp.concatenate([m] * (ROWS // 128), axis=1))
            s_s[kb] = p
            l_s[...] += lanes(jnp.add, p)

    def attend_values(t):
        l_s[...] = jnp.broadcast_to(1.0 / jnp.sum(l_s[...], axis=-1, keepdims=True), l_s.shape)
        o_s[...] = jnp.zeros_like(o_s)

        for kb in range(t + 1):
            r = l_s[...]
            p = (s_s[kb] * jnp.concatenate([r] * (ROWS // 128), axis=1)).astype(BF16)
            o_s[...] += jnp.dot(p, v_ref[keys(kb), :], preferred_element_type=F32)
        for h in range(heads):
            om_s[:, pl.ds(h * HEAD_DIM, HEAD_DIM)] = o_s[pl.ds(h * ROWS, ROWS), :].astype(BF16)

    def mlp(t, j):
        loaded(t, L_MLP + j, wgu.at[:, pl.ds(0, 2 * TILE)])
        a = a_s[...]
        gate = jnp.dot(a, wgu[:, pl.ds(j * TILE, TILE)], preferred_element_type=F32)
        up = jnp.dot(a, wgu[:, pl.ds(ff + j * TILE, TILE)], preferred_element_type=F32)
        om_s[:, pl.ds(qw + j * TILE, TILE)] = (jax.nn.silu(gate) * up).astype(BF16)

    def out_half(t, which, kind):
        if which == 0:
            loaded(t, L_OUT, wod)
        om = om_s[...]
        rows = pl.ds(pl.multiple_of(t * ROWS, ROWS), ROWS)
        tiles = width // TILE // 2
        for j in range(which * tiles, (which + 1) * tiles):
            cols = pl.ds(j * TILE, TILE)
            part[rows, cols] = jnp.dot(om, wod[:, cols], preferred_element_type=F32).astype(BF16)
        copy(kind, t).start()

    def chip_sum(t, cols, got, *sends):
        copy(got, t).wait_recv()
        for i in range(4):
            n = half // 4
            rows = pl.ds(pl.multiple_of(t * ROWS + core * half + i * n, n), n)
            other = swap[pl.ds(pl.multiple_of(t * half + i * n, n), n), cols].astype(F32)
            part[rows, cols] = (part[rows, cols].astype(F32) + other).astype(BF16)
        for kind in sends:
            copy(kind, t).start()

    def pass_on(t, cols, got, out, c):
        copy(got, t).wait_recv()
        rows = rows_of(t, c)
        part[rows, cols] = (part[rows, cols].astype(F32) + fwd[slot(t), cols].astype(F32)).astype(BF16)
        copy(out, t).start()

    def finish(t):
        take(recv_sem.at[R_FIN, t], 2 * chunk)
        rows = rows_of(t, chip)
        total = (part[rows, :].astype(F32) + from_l[slot(t), :].astype(F32)) + from_r[slot(t), :].astype(F32)
        y_ref[rows, :] = (x_v[rows, :].astype(F32) + total).astype(BF16)
        for kind in (OUT_R, OUT_L, OUT_P):
            copy(kind, t).start()

    last = blocks - 1

    def spread(t):
        take(recv_sem.at[R_OUT, t], 2 * chunk)
        far_kinds = (FAR_R, FAR_L) if t < last else (FAR_R_HALF, FAR_L_HALF, END_RP, END_LP, END_R, END_L)
        for kind in far_kinds + (P_LEFT, P_RIGHT):
            copy(kind, t).start()

    def far(t):
        take(recv_sem.at[R_FAR, t], chunk if t < last else chunk // 2)
        for kind in (P_FAR_A, P_FAR_B) if t < last else (P_END_A, P_END_B):
            copy(kind, t).start()

    stages = {
        'chip_sum_a': lambda t: chip_sum(t, A, SWAP_A, *((FWD_R,) if t in FWD_FIRST else (FWD_R, OWN_L))),
        'chip_sum_b': lambda t: chip_sum(t, B, SWAP_B, *((FWD_L, OWN_R, OWN_L) if t in FWD_FIRST else (FWD_L, OWN_R))),
        'pass_on_a': lambda t: pass_on(t, A, FWD_R, SUM_R, c_r),
        'pass_on_b': lambda t: pass_on(t, B, FWD_L, SUM_L, c_l),
        'finish': finish, 'spread': spread, 'far': far,
    }

    def place(p, s):
        for name, t in PLACES.get((s, p), ()):
            stages[name](t)

    def step(s):
        parts = {'project': lambda: project(s), 'scores': lambda: attend_scores(s), 'values': lambda: attend_values(s)}
        parts.update(('mlp%d' % j, functools.partial(mlp, s, j)) for j in range(ff_tiles))
        mlp_parts = ['mlp%d' % j for j in range(ff_tiles)]
        order = ['project', mlp_parts[0], 'scores'] + mlp_parts[1:-1] + ['values', mlp_parts[-1]]
        place('start', s)
        for name in order:
            parts[name]()
            place(name, s)
        if s == 0:
            pl.semaphore_wait(barrier, 5)
        out_half(s, 0, SWAP_A)
        place('out0', s)
        out_half(s, 1, SWAP_B)
        place('out1', s)

    for s in range(blocks):
        step(s)
    for name, t in DRAIN:
        stages[name](t)
    take(done_sem.at[0], tokens // 2 + chunk // 2)
    take(send_sem.at[S_SWAP], tokens // 2)
    take(send_sem.at[S_LINK], tokens * 3 // 4 + chunk // 2)
    take(send_sem.at[S_PARTNER], tokens // 2 - chunk // 2)


def store_kernel(y_ref, k_ref, v_ref, y_hbm, k_hbm, v_hbm, sem):
    n = y_ref.shape[0] // STORES
    copies = [pltpu.make_async_copy(y_ref.at[pl.ds(i * n, n)], y_hbm.at[pl.ds(i * n, n)], sem.at[2 + i])
              for i in range(STORES)]
    copies += [pltpu.make_async_copy(k_ref, k_hbm, sem.at[0]), pltpu.make_async_copy(v_ref, v_hbm, sem.at[1])]
    for cp in copies:
        cp.start()
    for cp in copies:
        cp.wait()


def solution(mesh):
    n_tp = mesh.shape['tp']

    def local_layer(x_in, g_norm, w_q, w_k, w_v, w_o, w_gate, w_up, w_down):
        tokens, width = x_in.shape
        blocks = tokens // ROWS
        qw, ff = w_q.shape[1], w_gate.shape[1]
        heads = qw // HEAD_DIM
        half = ROWS // 2
        chunk = half // (n_tp // 2)
        cos_r, sin_r, cos_t, sin_t = rope_constants(ROWS, blocks)
        rope = np.stack([np.concatenate([cos_r, cos_t]), np.concatenate([sin_r, sin_t])])
        rope = jnp.asarray(np.pad(rope, ((0, 0), (0, -blocks % 8), (0, 0))))
        vm = lambda: pl.BlockSpec(memory_space=pltpu.VMEM)
        hbm = lambda: pl.BlockSpec(memory_space=pl.ANY)
        y_out, k_rot, v_proj = pl.pallas_call(
            functools.partial(layer_kernel, n_tp),
            out_shape=(pltpu.VMEM((tokens, width), BF16),
                       pltpu.VMEM((tokens, HEAD_DIM), BF16),
                       pltpu.VMEM((tokens, HEAD_DIM), BF16)),
            in_specs=[hbm()] * 10,
            out_specs=(vm(), vm(), vm()),
            scratch_shapes=[
                pltpu.VMEM((tokens, width), BF16),
                pltpu.VMEM((width,), BF16),
                pltpu.VMEM(rope.shape, F32),
                pltpu.VMEM((width, qw + 2 * HEAD_DIM), BF16),
                pltpu.VMEM((width, 2 * ff), BF16),
                pltpu.VMEM((qw + ff, width), BF16),
                pltpu.VMEM((ROWS, width), BF16),
                pltpu.VMEM((heads * ROWS, HEAD_DIM), BF16),
                pltpu.VMEM((tokens // ROWS, heads * ROWS, ROWS), F32),
                pltpu.VMEM((heads * ROWS, 128), F32),
                pltpu.VMEM((heads * ROWS, 128), F32),
                pltpu.VMEM((heads * ROWS, HEAD_DIM), F32),
                pltpu.VMEM((ROWS, qw + ff), BF16),
                pltpu.VMEM((tokens, width), BF16),
                pltpu.VMEM((tokens // 2, width), BF16),
                pltpu.VMEM((blocks * chunk, width), BF16),
                pltpu.VMEM((blocks * chunk, width), BF16),
                pltpu.VMEM((blocks * chunk, width), BF16),
                pltpu.SemaphoreType.DMA((4 + ff // TILE + blocks,)),
                pltpu.SemaphoreType.DMA((3,)),
                pltpu.SemaphoreType.DMA((N_RECV, blocks)),
                pltpu.SemaphoreType.DMA((1,)),
            ],
            compiler_params=pltpu.CompilerParams(
                collective_id=0, has_side_effects=True, vmem_limit_bytes=52 * 2**20),
            name='layer',
        )(x_in, g_norm, w_q, w_k, w_v, w_o, w_gate, w_up, w_down, rope)
        y_out, k_rot, v_proj = pl.pallas_call(
            store_kernel,
            out_shape=tuple(jax.ShapeDtypeStruct(a.shape, BF16) for a in (y_out, k_rot, v_proj)),
            in_specs=[vm()] * 3, out_specs=(hbm(),) * 3,
            scratch_shapes=[pltpu.SemaphoreType.DMA((2 + STORES,))],
            compiler_params=pltpu.CompilerParams(vmem_limit_bytes=8 * 2**20),
            name='store',
        )(y_out, k_rot, v_proj)
        return y_out, k_rot.reshape(tokens, 1, HEAD_DIM), v_proj.reshape(tokens, 1, HEAD_DIM)

    return jax.shard_map(local_layer, mesh=mesh, in_specs=(P('dp', None), P(None), P(None, 'tp'), P(None, None), P(None, None), P('tp', None), P(None, 'tp'), P(None, 'tp'), P('tp', None)), out_specs=(P('dp', None), P('dp', 'tp', None), P('dp', 'tp', None)), check_vma=False)
```
